128 devices in a mesh: row: 8 (over x, core), col: 16 (over z, y).
Axes of the slice: x: 4, y: 4, z: 4, core: 2. Of those that a mesh axis runs over, the one named last changes fastest.
Arguments:
- fock_matrix: float32 [4096, 4096], P('row', 'col'), as said below
- density: float32 [4096, 4096], P('row', 'col'), as said below
- basis_gram: float32 [4096, 4096], P('row', 'col'), as said below
- error_history: float32 [6, 4096, 4096], P(None, 'row', 'col'), as said below
- fock_history: float32 [6, 4096, 4096], P(None, 'row', 'col'), may hold values from -6 to 6
Outputs:
- fock_next: float32 [4096, 4096], P('row', 'col')
- error_new: float32 [4096, 4096], P('row', 'col')
- weights: float32 [7], replicated
The draws below stay inside these ranges and needn't reach their ends.
Inputs may be any that keep to these rules, and one draw needn't show every extreme that they name: `fock_matrix`: symmetric. `density`: symmetric. `basis_gram`: symmetric. `error_history`: each of the 6 matrices is antisymmetric.
All inputs are finite; a program needn't handle non-finite values.
Results may differ from the reference program's by a relative error of at most 0.000098.
Values sent between devices are 32-bit elements; how exact they have to be, the bound alone decides.
A program may use at most 128 MiB of HBM per device.

```python
import jax
import jax.numpy as jnp
from jax import lax

N = 4096
HIST = 6


def draw_fock_matrix(key, part):
    base = jax.random.normal(jax.random.fold_in(key, 11), (N, N), jnp.float32)
    return (base + base.T) * 0.7071


def draw_density(key, part):
    base = jax.random.normal(jax.random.fold_in(key, 21), (N, N), jnp.float32)
    return (base + base.T) * (0.7071 / N ** 0.5)


def draw_basis_gram(key, part):
    base = jax.random.normal(jax.random.fold_in(key, 31), (N, N), jnp.float32)
    return jnp.eye(N, dtype=jnp.float32) + (base + base.T) * (0.35 / N ** 0.5)


def draw_error_history(key, part):
    common = jax.random.normal(jax.random.fold_in(key, 41), (N, N), jnp.float32)
    own = jax.random.normal(jax.random.fold_in(key, 42), (HIST, N, N), jnp.float32)
    spread = 0.7
    scales = jnp.exp(jax.random.uniform(jax.random.fold_in(key, 43), (HIST, 1, 1), jnp.float32, -spread, spread))
    mixed = (0.6 * common[None] + 0.8 * own) * scales
    return (mixed - jnp.swapaxes(mixed, 1, 2)) * 0.7071


def levels(rng, dims, shards, low, high):
    factor_of, own = 1.0, jax.random.fold_in(rng, 6)
    for position, parts in shards:
        steps = jnp.exp(jax.random.uniform(jax.random.fold_in(own, position), (parts,), jnp.float32, low / len(shards), high / len(shards)))
        factor_of = factor_of * jnp.repeat(steps, dims[position] // parts).reshape([-1 if axis == position else 1 for axis in range(len(dims))])
    return factor_of


def normal_values(stream_key, dims, width, most, pieces=(), kind=jnp.bfloat16):
    values = jax.random.normal(stream_key, dims, jnp.float32) * width
    if len(pieces) > 0:
        values = levels(stream_key, dims, pieces, -0.22, 0.18) * values
    return jnp.clip(values, min=-most, max=most).astype(kind)


def setup_inputs(seed: int = 0) -> dict:
    key_of = jax.random.split(jax.random.key(seed), 6)
    return {
        "fock_matrix": draw_fock_matrix(jax.random.fold_in(key_of[5], 71), 0),
        "density": draw_density(jax.random.fold_in(key_of[5], 71), 0),
        "basis_gram": draw_basis_gram(jax.random.fold_in(key_of[5], 71), 0),
        "error_history": draw_error_history(jax.random.fold_in(key_of[5], 71), 0),
        "fock_history": normal_values(key_of[4], (HIST, N, N), 1.0, 6.0, ((1, 8), (2, 16)), jnp.float32),
    }


def solve_weights(gram):
    size = gram.shape[0]
    factor = jnp.linalg.cholesky(gram)
    forward = []
    for index in range(size):
        total = jnp.float32(1.0)
        for inner in range(index):
            total = total - factor[index, inner] * forward[inner]
        forward.append(total / factor[index, index])
    backward = [None] * size
    for index in range(size - 1, -1, -1):
        total = forward[index]
        for inner in range(index + 1, size):
            total = total - factor[inner, index] * backward[inner]
        backward[index] = total / factor[index, index]
    solved = jnp.stack(backward)
    return solved / jnp.sum(solved)

def reference(fock_matrix, density, basis_gram, error_history, fock_history):
    highest = lax.Precision.HIGHEST
    middle = jnp.dot(density.astype(jnp.float32), basis_gram.astype(jnp.float32), precision=highest, preferred_element_type=jnp.float32)
    product = jnp.dot(fock_matrix.astype(jnp.float32), middle.astype(jnp.float32), precision=highest, preferred_element_type=jnp.float32)
    error_new = product - product.T
    stacked = jnp.concatenate([error_history, error_new[None]], axis=0)
    gram = jnp.einsum('kij,lij->kl', stacked, stacked, precision=highest)
    weights = solve_weights(gram)
    fock_next = jnp.einsum('k,kij->ij', weights[:HIST], fock_history, precision=highest) + weights[HIST] * fock_matrix
    return (fock_next, error_new, weights)
```

```python
import jax
import jax.numpy as jnp
from jax import lax
from jax.experimental import pallas as pl
from jax.experimental.pallas import tpu as pltpu
from jax.sharding import Mesh
from jax.sharding import PartitionSpec as P

MESH = pl.DeviceIdType.MESH
F32 = jnp.float32
BF16 = jnp.bfloat16
UNITS = (((0, 0), (0, 1)), ((1, 0), (2, 1)), ((1, 1), (2, 0)), ((3, 0), (3, 1)))
NS, NU = 2, 4
NCOPY = 240
PAIRS = [(a, b) for a in range(6) for b in range(a, 6)]


def split(v):
    hi = v.astype(BF16)
    return hi, (v - hi.astype(F32)).astype(BF16)


def dot3(a_hi, a_lo, b_hi, b_lo):
    a = jnp.concatenate([a_hi, a_hi, a_lo], axis=1)
    b = jnp.concatenate([b_hi, b_lo, b_hi], axis=0)
    return jnp.dot(a, b, preferred_element_type=F32)


def kernel(
    f_hbm, d_hbm, s_hbm, eh_hbm, fh_hbm, next_hbm, err_hbm, w_ref,
    dg, sg, fg, dt_hi, dt_lo, s_hi, s_lo, f_hi, f_lo,
    mp, dx, ra, rb, fl, fr, mf, pacc, za, zb, zl, zr, pf, tb,
    eh, fh, err, out, red_y, red_z, red_x,
    send_sem, recv_sem, local_sem, t_send, t_recv,
):
    x, c, z, y = (lax.axis_index(n) for n in ("x", "c", "z", "y"))
    xr, xl, xo = lax.rem(x + 1, 4), lax.rem(x + 3, 4), lax.rem(x + 2, 4)
    dev = lambda x=x, c=c, z=z, y=y: (x, c, z, y)
    x_right, x_left = dev(x=xr), dev(x=xl)
    y_right, y_left = dev(y=lax.rem(y + 1, 4)), dev(y=lax.rem(y + 3, 4))
    z_right, z_left = dev(z=lax.rem(z + 1, 4)), dev(z=lax.rem(z + 3, 4))
    oc = 1 - c
    partner = dev(c=oc)

    sent = []

    def send(src, dst, to):
        k = len(sent)
        copy = pltpu.make_async_remote_copy(
            src_ref=src, dst_ref=dst, send_sem=send_sem.at[k], recv_sem=recv_sem.at[k],
            device_id=to, device_id_type=MESH,
        )
        copy.start()
        sent.append(copy)
        return copy

    local = []

    def load(src, dst):
        copy = pltpu.make_async_copy(src, dst, local_sem.at[len(local)])
        copy.start()
        local.append(copy)
        return copy

    def cols(ref, h):
        return ref.at[:, pl.ds(128 * h, 128)]

    load_d = [load(cols(d_hbm, h), dg.at[0, h]) for h in range(2)]
    load_s = [load(cols(s_hbm, h), sg.at[0, h]) for h in range(2)]
    load_f = [load(cols(f_hbm, h), fg.at[0, h]) for h in range(2)]
    load_e = load(eh_hbm, eh)
    load_h = load(fh_hbm, fh)

    barrier = pltpu.get_barrier_semaphore()
    for to in (x_right, x_left, y_right, y_left, z_right, z_left, partner):
        pl.semaphore_signal(barrier, inc=1, device_id=to, device_id_type=MESH)
    pl.semaphore_wait(barrier, 7)

    def y_sends(src, g):
        r0 = send(cols(src, 0), g.at[1, 0], y_right)
        l1 = send(cols(src, 1), g.at[2, 1], y_left)
        r1 = send(cols(src, 1), g.at[1, 1], y_right)
        l0 = send(cols(src, 0), g.at[2, 0], y_left)
        return r0, l1, r1, l0

    def y_forward(first, g):
        first[0].wait_recv()
        r = send(g.at[1, 0], g.at[3, 0], y_right)
        first[1].wait_recv()
        l = send(g.at[2, 1], g.at[3, 1], y_left)
        return r, l

    LO, HI = pl.ds(0, 256), pl.ds(256, 256)

    def z_sends(s):
        src = lambda rows: s_hbm.at[rows, pl.ds(128 * s, 128)]
        r0 = send(src(LO), sg.at[1, s, LO], z_right)
        l1 = send(src(HI), sg.at[2, s, HI], z_left)
        r1 = send(src(HI), sg.at[1, s, HI], z_right)
        l0 = send(src(LO), sg.at[2, s, LO], z_left)
        return r0, l1, r1, l0

    def z_forward(first, s):
        first[0].wait_recv()
        r = send(sg.at[1, s, LO], sg.at[3, s, LO], z_right)
        first[1].wait_recv()
        l = send(sg.at[2, s, HI], sg.at[3, s, HI], z_left)
        return r, l

    def prep_s(s, slots):
        for slot in slots:
            hi, lo = split(sg[slot, s])
            at = pl.ds(128 * slot, 128)
            s_hi[s, :, at] = hi
            s_lo[s, :, at] = lo

    def prep_d(u):
        for n, (slot, h) in enumerate(UNITS[u]):
            for k in range(4):
                hi, lo = split(dg[slot, h, pl.ds(128 * k, 128), :].T)
                dt_hi[u, pl.ds(128 * n, 128), pl.ds(128 * k, 128)] = hi
                dt_lo[u, pl.ds(128 * n, 128), pl.ds(128 * k, 128)] = lo

    def prep_f(u):
        for n, (slot, h) in enumerate(UNITS[u]):
            hi, lo = split(fg[slot, h])
            f_hi[u, :, pl.ds(128 * n, 128)] = hi
            f_lo[u, :, pl.ds(128 * n, 128)] = lo

    ALL, TOP, LOW = pl.ds(0, 32), pl.ds(0, 16), pl.ds(16, 16)
    g = [dict() for _ in range(NS * NU)]

    def p0(t):
        s, u = divmod(t, NU)
        tile = dot3(dt_hi[u], dt_lo[u], s_hi[s], s_lo[s])
        for k in range(2):
            for q in range(4):
                mp[t, k, q] = tile[(k * 4 + q) * 32 : (k * 4 + q + 1) * 32]
        g[t]["dx"] = send(mp.at[t, oc], dx.at[t], partner)

    def p1(t):
        g[t]["dx"].wait_recv()
        for q in range(4):
            mp[t, c, q] += dx[t, q]
        g[t]["ra"] = send(mp.at[t, c, xo, TOP], ra.at[t], x_right)
        g[t]["rb"] = send(mp.at[t, c, xo, LOW], rb.at[t], x_left)
        g[t]["fl1"] = send(mp.at[t, c, xr, LOW], fl.at[t, LOW], x_right)
        g[t]["fr0"] = send(mp.at[t, c, xl, TOP], fr.at[t, TOP], x_left)

    def p2(t):
        g[t]["ra"].wait_recv()
        mp[t, c, xr, TOP] += ra[t]
        g[t]["fl0"] = send(mp.at[t, c, xr, TOP], fl.at[t, TOP], x_right)
        g[t]["rb"].wait_recv()
        mp[t, c, xl, LOW] += rb[t]
        g[t]["fr1"] = send(mp.at[t, c, xl, LOW], fr.at[t, LOW], x_left)

    def p3(t):
        for name in ("fl1", "fr0", "fl0", "fr1"):
            g[t][name].wait_recv()
        mf[t, c, x] = mp[t, c, x] + fl[t] + fr[t]
        top, low = mf.at[t, c, x, TOP], mf.at[t, c, x, LOW]
        g[t]["gr0"] = send(top, top, x_right)
        g[t]["gl1"] = send(low, low, x_left)
        g[t]["gr1"] = send(low, low, x_right)
        g[t]["gl0"] = send(top, top, x_left)
        g[t]["gp"] = send(mf.at[t, c, x], mf.at[t, c, x], partner)

    def p4(t):
        g[t]["gr0"].wait_recv()
        g[t]["hr"] = send(mf.at[t, c, xl, TOP], mf.at[t, c, xl, TOP], x_right)
        g[t]["gl1"].wait_recv()
        g[t]["hl"] = send(mf.at[t, c, xr, LOW], mf.at[t, c, xr, LOW], x_left)
        g[t]["gr1"].wait_recv()
        g[t]["ql"] = send(mf.at[t, c, xl], mf.at[t, c, xl], partner)
        g[t]["gl0"].wait_recv()
        g[t]["qr"] = send(mf.at[t, c, xr], mf.at[t, c, xr], partner)

    def p5(t):
        g[t]["hr"].wait_recv()
        g[t]["hl"].wait_recv()
        g[t]["qo"] = send(mf.at[t, c, xo], mf.at[t, c, xo], partner)

    def p6(t):
        s, u = divmod(t, NU)
        for name in ("gp", "ql", "qr", "qo"):
            g[t][name].wait_recv()
        m_hi, m_lo = split(jnp.concatenate([mf[t, k, q] for k in range(2) for q in range(4)], axis=0))
        part = dot3(f_hi[u], f_lo[u], m_hi, m_lo)
        for slot in range(4):
            piece = part[:, 128 * slot : 128 * (slot + 1)]
            if u == 0:
                pacc[s, slot] = piece
            else:
                pacc[s, slot] += piece

    w = [dict() for _ in range(NS)]

    def z1(s):
        w[s]["za"] = send(pacc.at[s, 3, LO], za.at[s], z_right)
        w[s]["zb"] = send(pacc.at[s, 3, HI], zb.at[s], z_left)
        w[s]["zl1"] = send(pacc.at[s, 2, HI], zl.at[s, HI], z_right)
        w[s]["zr0"] = send(pacc.at[s, 1, LO], zr.at[s, LO], z_left)

    def z2(s):
        w[s]["za"].wait_recv()
        pacc[s, 2, LO] += za[s]
        w[s]["zl0"] = send(pacc.at[s, 2, LO], zl.at[s, LO], z_right)
        w[s]["zb"].wait_recv()
        pacc[s, 1, HI] += zb[s]
        w[s]["zr1"] = send(pacc.at[s, 1, HI], zr.at[s, HI], z_left)

    own_half = lax.rem(y, 2)
    t_core = lax.div(y, 2)
    mirror = jnp.logical_and(x == z, c == t_core)

    def t_copy(s, h):
        return pltpu.make_async_remote_copy(
            src_ref=pf.at[s, pl.ds(256 * h, 256)], dst_ref=tb.at[own_half, s],
            send_sem=t_send.at[s, h], recv_sem=t_recv.at[s, own_half],
            device_id=(z, t_core, x, 2 * c + h), device_id_type=MESH,
        )

    def t_local(s, h):
        return pltpu.make_async_copy(pf.at[s, pl.ds(256 * h, 256)], tb.at[own_half, s], t_recv.at[s, own_half])

    def z3(s):
        for name in ("zl1", "zr0", "zl0", "zr1"):
            w[s][name].wait_recv()
        pf[s] = pacc[s, 0] + zl[s] + zr[s]
        for h in range(2):
            mine = jnp.logical_and(mirror, own_half == h)

            @pl.when(mine)
            def _():
                t_local(s, h).start()

            @pl.when(jnp.logical_not(mine))
            def _():
                t_copy(s, h).start()

    def t_wait(s, half):
        pltpu.make_async_copy(pf.at[s, LO], tb.at[half, s], t_recv.at[s, half]).wait()

    def history_gram():
        def step(n, acc):
            rows = pl.ds(pl.multiple_of(8 * n, 8), 8)
            acc = list(acc)
            for col in range(2):
                e = [eh[k, rows, pl.ds(128 * col, 128)] for k in range(6)]
                acc = [v + e[a] * e[b] for v, (a, b) in zip(acc, PAIRS)]
            return tuple(acc)

        acc = lax.fori_loop(0, 64, step, tuple(jnp.zeros((8, 128), F32) for _ in PAIRS))
        return [jnp.sum(v, axis=0, keepdims=True) for v in acc]

    d_first = y_sends(d_hbm, dg)
    s_first = [z_sends(0)]
    for n in load_d + load_s:
        n.wait()
    prep_d(0)
    for s in range(NS):
        prep_s(s, (0,))
    load_e.wait()
    hist = history_gram()
    s_fwd = [z_forward(s_first[0], 0)]
    s_first.append(z_sends(1))
    d_fwd = y_forward(d_first, dg)
    f_first = y_sends(f_hbm, fg)
    prep_d(1)
    s_first[0][2].wait_recv()
    s_first[0][3].wait_recv()
    prep_s(0, (1, 2))
    s_fwd[0][0].wait_recv()
    s_fwd[0][1].wait_recv()
    prep_s(0, (3,))
    p0(0)
    p0(1)
    p1(0)
    p1(1)
    s_fwd.append(z_forward(s_first[1], 1))
    d_first[2].wait_recv()
    d_first[3].wait_recv()
    prep_d(2)
    p0(2)
    p2(0)
    p2(1)
    p1(2)
    p3(0)
    p3(1)
    d_fwd[0].wait_recv()
    d_fwd[1].wait_recv()
    prep_d(3)
    p0(3)
    p2(2)
    p1(3)
    p4(0)
    s_first[1][2].wait_recv()
    s_first[1][3].wait_recv()
    prep_s(1, (1, 2))
    s_fwd[1][0].wait_recv()
    s_fwd[1][1].wait_recv()
    prep_s(1, (3,))
    p0(4)
    p4(1)
    p3(2)
    p2(3)
    p1(4)
    f_fwd = y_forward(f_first, fg)
    for n in load_f:
        n.wait()
    prep_f(0)
    p0(5)
    p5(0)
    p5(1)
    p6(0)
    p4(2)
    p3(3)
    p2(4)
    p1(5)
    prep_f(1)
    p0(6)
    p6(1)
    p5(2)
    p4(3)
    p3(4)
    p2(5)
    p1(6)
    f_first[2].wait_recv()
    f_first[3].wait_recv()
    prep_f(2)
    p0(7)
    p6(2)
    p5(3)
    p4(4)
    p3(5)
    p2(6)
    p1(7)
    f_fwd[0].wait_recv()
    f_fwd[1].wait_recv()
    prep_f(3)
    p6(3)
    z1(0)
    p5(4)
    p4(5)
    p3(6)
    p2(7)
    p6(4)
    p5(5)
    p4(6)
    p3(7)
    z2(0)
    p6(5)
    p5(6)
    p4(7)
    p6(6)
    p5(7)
    p6(7)
    z1(1)
    z3(0)
    z2(1)
    z3(1)

    sums = [jnp.zeros((8, 128), F32) for _ in range(7)]
    load_h.wait()
    for half in range(2):
        for s in range(NS):
            t_wait(s, half)
            start = 256 * half + 128 * s
            rows = pl.ds(start, 128)
            for col in range(2):
                at = pl.ds(128 * col, 128)
                err[rows, at] = pf[col, rows, :] - tb[half, s, at, :].T

            def step(n, acc):
                at = pl.ds(pl.multiple_of(start + 8 * n, 8), 8)
                for col in range(2):
                    lanes = pl.ds(128 * col, 128)
                    e = err[at, lanes]
                    acc = tuple(acc[k] + eh[k, at, lanes] * e for k in range(6)) + (acc[6] + e * e,)
                return acc

            sums = lax.fori_loop(0, 16, step, tuple(sums))
    err_out = load(err, err_hbm)

    top = hist + [jnp.sum(v, axis=0, keepdims=True) for v in sums] + [jnp.zeros((4, 128), F32)]
    red_y[y] = jnp.concatenate(top, axis=0)
    for d in range(1, 4):
        send(red_y.at[y], red_y.at[y], dev(y=lax.rem(y + d, 4)))
    for copy in sent[-3:]:
        copy.wait_recv()
    red_z[z] = red_y[0] + red_y[1] + red_y[2] + red_y[3]
    for d in range(1, 4):
        send(red_z.at[z], red_z.at[z], dev(z=lax.rem(z + d, 4)))
    for copy in sent[-3:]:
        copy.wait_recv()
    me = 2 * x + c
    red_x[me] = red_z[0] + red_z[1] + red_z[2] + red_z[3]
    for d in range(1, 8):
        to = lax.rem(me + d, 8)
        send(red_x.at[me], red_x.at[me], dev(x=lax.div(to, 2), c=lax.rem(to, 2)))
    for copy in sent[-7:]:
        copy.wait_recv()
    total = red_x[0]
    for k in range(1, 8):
        total = total + red_x[k]
    total = jnp.broadcast_to(jnp.sum(total, axis=1, keepdims=True), (32, 128))

    gram = {}
    for n, (a, b) in enumerate(PAIRS):
        gram[b, a] = total[n : n + 1]
    for k in range(7):
        gram[6, k] = total[21 + k : 22 + k]
    low = {}
    for j in range(7):
        v = gram[j, j]
        for k in range(j):
            v = v - low[j, k] * low[j, k]
        low[j, j] = jnp.sqrt(v)
        for i in range(j + 1, 7):
            v = gram[i, j]
            for k in range(j):
                v = v - low[i, k] * low[j, k]
            low[i, j] = v / low[j, j]
    forward = []
    for i in range(7):
        v = jnp.ones((1, 128), F32)
        for k in range(i):
            v = v - low[i, k] * forward[k]
        forward.append(v / low[i, i])
    backward = [None] * 7
    for i in range(6, -1, -1):
        v = forward[i]
        for k in range(i + 1, 7):
            v = v - low[k, i] * backward[k]
        backward[i] = v / low[i, i]
    norm = backward[0]
    for v in backward[1:]:
        norm = norm + v
    weights = [v / norm for v in backward]
    lane = lax.broadcasted_iota(jnp.int32, (1, 128), 1)
    row = jnp.zeros((1, 128), F32)
    for k in range(7):
        row = jnp.where(lane == k, weights[k], row)
    w_ref[...] = row
    spread = [jnp.broadcast_to(v, (8, 128)) for v in weights]

    def mix(n, carry):
        at = pl.ds(pl.multiple_of(8 * n, 8), 8)
        for col in range(2):
            lanes = pl.ds(128 * col, 128)
            v = spread[6] * fg[0, col, at, :]
            for k in range(6):
                v = v + spread[k] * fh[k, at, lanes]
            out[at, lanes] = v
        return carry

    lax.fori_loop(0, 64, mix, 0)
    next_out = load(out, next_hbm)
    for copy in sent:
        copy.wait_send()
    for s in range(NS):
        for h in range(2):

            @pl.when(jnp.logical_not(jnp.logical_and(mirror, own_half == h)))
            def _():
                t_copy(s, h).wait_send()

    err_out.wait()
    next_out.wait()


def body(fock_matrix, density, basis_gram, error_history, fock_history):
    any_ = pl.BlockSpec(memory_space=pl.ANY)
    v = pltpu.VMEM
    block = jax.ShapeDtypeStruct((512, 256), F32)
    next_, err, w = pl.pallas_call(
        kernel,
        out_shape=(block, block, jax.ShapeDtypeStruct((1, 128), F32)),
        in_specs=[any_] * 5,
        out_specs=(any_, any_, pl.BlockSpec(memory_space=pltpu.VMEM)),
        scratch_shapes=[
            v((4, 2, 512, 128), F32), v((4, 2, 512, 128), F32), v((4, 2, 512, 128), F32),
            v((4, 256, 512), BF16), v((4, 256, 512), BF16),
            v((2, 512, 512), BF16), v((2, 512, 512), BF16),
            v((4, 512, 256), BF16), v((4, 512, 256), BF16),
            v((8, 2, 4, 32, 512), F32), v((8, 4, 32, 512), F32),
            v((8, 16, 512), F32), v((8, 16, 512), F32),
            v((8, 32, 512), F32), v((8, 32, 512), F32),
            v((8, 2, 4, 32, 512), F32),
            v((2, 4, 512, 128), F32),
            v((2, 256, 128), F32), v((2, 256, 128), F32),
            v((2, 512, 128), F32), v((2, 512, 128), F32),
            v((2, 512, 128), F32),
            v((2, 2, 256, 128), F32),
            v((6, 512, 256), F32), v((6, 512, 256), F32),
            v((512, 256), F32), v((512, 256), F32),
            v((4, 32, 128), F32), v((4, 32, 128), F32), v((8, 32, 128), F32),
            pltpu.SemaphoreType.DMA((NCOPY,)), pltpu.SemaphoreType.DMA((NCOPY,)),
            pltpu.SemaphoreType.DMA((10,)),
            pltpu.SemaphoreType.DMA((2, 2)), pltpu.SemaphoreType.DMA((2, 2)),
        ],
        compiler_params=pltpu.CompilerParams(
            collective_id=0, has_side_effects=True, vmem_limit_bytes=60 * 1024 * 1024
        ),
    )(fock_matrix, density, basis_gram, error_history, fock_history)
    return next_, err, w[0, :7]


def solution(mesh):
    split_mesh = Mesh(mesh.devices.reshape(4, 2, 4, 4), ("x", "c", "z", "y"))
    two = P(("x", "c"), ("z", "y"))
    three = P(None, ("x", "c"), ("z", "y"))
    return jax.shard_map(
        body,
        mesh=split_mesh,
        in_specs=(two, two, two, three, three),
        out_specs=(two, two, P()),
        check_vma=False,
    )
```

```python
import jax
import jax.numpy as jnp
from jax import lax
from jax.experimental import pallas as pl
from jax.experimental.pallas import tpu as pltpu
from jax.sharding import Mesh
from jax.sharding import PartitionSpec as P

MESH = pl.DeviceIdType.MESH
F32 = jnp.float32
BF16 = jnp.bfloat16
UNITS = (((0, 0), (0, 1)), ((1, 0), (2, 1)), ((1, 1), (2, 0)), ((3, 0), (3, 1)))
NS, NU = 4, 4
PAIRS = [(a, b) for a in range(6) for b in range(a, 6)]
GROUPS = (
    (0, 0, 1),
    (0, 1, 1),
    (1, 0, 2),
    (0, 2, 1),
    (1, 2, 1),
    (2, 0, 2),
    (0, 3, 1),
    (1, 3, 1),
    (2, 2, 2),
    (3, 0, 2),
    (3, 2, 2),
)
ORDER = (
    ("ys", 0), ("zs", 0), ("pd", 0), ("hist", 0), ("zf", 0), ("zs", 1), ("ps", 0), ("p0", 0), ("zf", 1), ("zs", 2),
    ("yf", 0), ("fs", 0), ("pd", 1), ("p0", 1), ("p1", 0), ("pf", 0, 0), ("pf", 0, 1), ("p1", 1), ("p2", 0),
    ("ps", 1), ("p0", 2), ("p2", 1), ("zf", 2), ("zs", 3), ("pd", 2), ("p0", 3), ("p1", 2), ("p0", 4), ("p3", 0),
    ("p1", 3), ("p3", 1), ("p1", 4), ("ps", 2), ("p0", 5), ("p2", 2), ("pd", 3), ("p0", 6), ("zf", 3), ("p0", 7),
    ("p4", 0), ("p1", 5), ("p2", 3), ("p0", 8), ("p1", 6), ("p4", 1), ("p1", 7), ("p2", 4), ("p3", 2), ("ff", 0),
    ("fs", 1), ("p1", 8), ("p5", 0), ("pf", 1, 0), ("ps", 3), ("p0", 9), ("p6", 0, 0), ("p6", 0, 1), ("p2", 5),
    ("p2", 6), ("p0", 10), ("p5", 1), ("p1", 9), ("p2", 7), ("pf", 2, 0), ("p3", 3), ("p3", 4), ("p1", 10),
    ("p6", 1, 0), ("pf", 3, 0), ("p4", 2), ("p2", 8), ("p3", 5), ("p3", 6), ("p2", 9), ("ff", 1), ("pf", 1, 1),
    ("p6", 1, 1), ("p3", 7), ("p4", 3), ("p4", 4), ("p2", 10), ("pf", 2, 1), ("p5", 2), ("p3", 8), ("p6", 2, 0),
    ("p6", 2, 1), ("p4", 5), ("pf", 3, 1), ("p4", 6), ("p3", 9), ("p4", 7), ("p5", 3), ("p5", 4), ("p3", 10),
    ("p6", 3, 0), ("p6", 3, 1), ("p6", 4, 0), ("p6", 4, 1), ("p4", 8), ("p5", 5), ("p5", 6), ("p6", 5, 0),
    ("p6", 5, 1), ("p4", 9), ("p5", 7), ("p6", 6, 0), ("p6", 6, 1), ("z1", 0, 0), ("z1", 0, 1), ("p4", 10),
    ("p6", 7, 0), ("p6", 7, 1), ("p5", 8), ("z1", 1, 0), ("z1", 1, 1), ("p5", 9), ("p6", 8, 0), ("p6", 8, 1),
    ("z2", 0, 0), ("p6", 9, 0), ("p5", 10), ("p6", 9, 1), ("z2", 0, 1), ("z1", 2, 0), ("z1", 2, 1), ("p6", 10, 0),
    ("p6", 10, 1), ("z2", 1, 0), ("z1", 3, 0), ("z1", 3, 1), ("z2", 1, 1), ("z3", 0, 0), ("ha",), ("z3", 0, 1),
    ("z2", 2, 0), ("z2", 2, 1), ("z3", 1, 0), ("z2", 3, 0), ("z2", 3, 1), ("z3", 1, 1), ("t", 0, 0), ("t", 0, 1),
    ("z3", 2, 0), ("hb",), ("z3", 2, 1), ("z3", 3, 0), ("z3", 3, 1), ("hc",), ("t", 2, 0), ("t", 2, 1),
)
N_RECV = 49 + 9 * len(GROUPS)
RELAYED = (0, 2)
RELAY_AXIS = "z"


def split(v):
    hi = v.astype(BF16)
    return hi, (v - hi.astype(F32)).astype(BF16)


def dot3(a_hi, a_lo, b_hi, b_lo):
    a = jnp.concatenate([a_hi, a_hi, a_lo], axis=1)
    b = jnp.concatenate([b_hi, b_lo, b_hi], axis=0)
    return jnp.dot(a, b, preferred_element_type=F32)


def kernel(
    f_hbm, d_hbm, s_hbm, eh_hbm, fh_hbm, next_hbm, err_hbm, w_ref,
    s_in, sg, dg, fg, s_hi, s_lo, d_hi, d_lo, f_hi, f_lo,
    mp, dx, ra, rb, flr, mf, m_hi, m_lo, pacc, za, zb, zlr, pf, tb, hop,
    eh, fh, own, err, out, ha, hb, na, nb,
    send_sem, recv_sem, local_sem, t_send, t_recv, hop_recv, hop_send,
):
    x, c, z, y = (lax.axis_index(n) for n in ("x", "c", "z", "y"))
    xr, xl, xo = lax.rem(x + 1, 4), lax.rem(x + 3, 4), lax.rem(x + 2, 4)
    dev = lambda x=x, c=c, z=z, y=y: (x, c, z, y)
    x_right, x_left = dev(x=xr), dev(x=xl)
    y_right, y_left = dev(y=lax.rem(y + 1, 4)), dev(y=lax.rem(y + 3, 4))
    z_right, z_left = dev(z=lax.rem(z + 1, 4)), dev(z=lax.rem(z + 3, 4))
    oc = 1 - c
    partner = dev(c=oc)

    used = {"send": 0, "recv": 0}
    outgoing = []

    def recv():
        used["recv"] += 1
        return recv_sem.at[used["recv"] - 1]

    def sender(*whole):
        used["send"] += len(whole)
        base = used["send"] - len(whole)
        for k, ref in enumerate(whole):
            outgoing.append((send_sem.at[base + k], ref))
        return [send_sem.at[base + k] for k in range(len(whole))]

    def send(src, dst, to, out_sem, in_sem):
        pltpu.make_async_remote_copy(
            src_ref=src, dst_ref=dst, send_sem=out_sem, recv_sem=in_sem, device_id=to, device_id_type=MESH,
        ).start()

    def wait(sem, ref):
        pltpu.make_async_copy(ref, ref, sem).wait()

    local = []

    def load(src, dst):
        copy = pltpu.make_async_copy(src, dst, local_sem.at[len(local)])
        copy.start()
        local.append(copy)
        return copy

    lanes = [pl.ds(0, 128), pl.ds(128, 128)]
    halves = [pl.ds(0, 256), pl.ds(256, 256)]

    barrier = pltpu.get_barrier_semaphore()
    for to in (x_right, x_left, y_right, y_left, z_right, z_left, partner):
        pl.semaphore_signal(barrier, inc=1, device_id=to, device_id_type=MESH)
    load_s = load(s_hbm, s_in)
    load_d = [load(d_hbm.at[:, lanes[h]], dg.at[0, h]) for h in range(2)]
    load_e = load(eh_hbm, eh)
    load_f = [load(f_hbm.at[halves[r], lanes[h]], fg.at[0, r, h]) for r in range(2) for h in range(2)]
    load_h = load(fh_hbm, fh)
    load_s.wait()
    for n in range(2):
        for k in range(4):
            block = s_in[pl.ds(128 * k, 128), lanes[n]].T
            for e in range(2):
                sg[0, 2 * n + e, :, pl.ds(128 * k, 128)] = block[64 * e : 64 * (e + 1)]
    pl.semaphore_wait(barrier, 7)

    three = pl.ds(0, 3)
    (d_out,) = sender(dg.at[three])
    (f_out,) = sender(fg.at[three])
    (s_out,) = sender(sg.at[three])

    class Line:
        def __init__(self, src, slot, size, right, left, out_sem):
            self.src, self.slot, self.size, self.right, self.left, self.out = src, slot, size, right, left, out_sem
            self.sems = [recv() for _ in range(3)]

        def begin(self):
            a, b, _ = self.sems
            send(self.src(0), self.slot(1, 0), self.right, self.out, a)
            send(self.src(1), self.slot(2, 1), self.left, self.out, a)
            send(self.src(1), self.slot(1, 1), self.right, self.out, b)
            send(self.src(0), self.slot(2, 0), self.left, self.out, b)

        def forward(self):
            wait(self.sems[0], self.size)
            send(self.slot(1, 0), self.slot(3, 0), self.right, self.out, self.sems[2])
            send(self.slot(2, 1), self.slot(3, 1), self.left, self.out, self.sems[2])

        def second(self):
            wait(self.sems[1], self.size)

        def third(self):
            wait(self.sems[2], self.size)

    d_line = Line(lambda h: d_hbm.at[:, lanes[h]], lambda slot, h: dg.at[slot, h], dg.at[1], y_right, y_left, d_out)
    f_line = [
        Line(
            lambda h, r=r: f_hbm.at[halves[r], lanes[h]], lambda slot, h, r=r: fg.at[slot, r, h],
            fg.at[1, r], y_right, y_left, f_out,
        )
        for r in range(2)
    ]

    LO, HI = pl.ds(0, 32), pl.ds(32, 32)
    part = (LO, HI)
    s_line = [
        Line(
            lambda h, s=s: sg.at[0, s, part[h]], lambda slot, h, s=s: sg.at[slot, s, part[h]],
            sg.at[1, s], z_right, z_left, s_out,
        )
        for s in range(NS)
    ]

    def prep_s(s, slots):
        for slot in slots:
            hi, lo = split(sg[slot, s])
            at = pl.ds(64 * slot, 64)
            s_hi[s, at, :] = hi
            s_lo[s, at, :] = lo

    def prep_d(u):
        for n, (slot, h) in enumerate(UNITS[u]):
            hi, lo = split(dg[slot, h])
            d_hi[u, :, lanes[n]] = hi
            d_lo[u, :, lanes[n]] = lo

    def prep_f(u, r):
        for n, (slot, h) in enumerate(UNITS[u]):
            for k in range(2):
                hi, lo = split(fg[slot, r, h, lanes[k], :].T)
                f_hi[u, r, lanes[n], lanes[k]] = hi
                f_lo[u, r, lanes[n], lanes[k]] = lo

    TOP, LOW = pl.ds(0, 16), pl.ds(16, 16)
    g = [dict() for _ in GROUPS]

    def at(n):
        s, first, count = GROUPS[n]
        return s, pl.ds(first, count), range(first, first + count)

    dx_out, ra_out, rb_out, f1_out, f0_out, g_right, g_left, h_out, q_out = sender(
        dx, ra, rb, flr.at[:, :, 0], flr.at[:, :, 1], flr.at[:, :, 0], flr.at[:, :, 0], flr.at[:, :, 0], dx
    )

    def p0(n):
        s, us, units = at(n)
        d = [jnp.concatenate([ref[u] for u in units], axis=1) for ref in (d_hi, d_lo)]
        tile = dot3(s_hi[s], s_lo[s], *d)
        for k, u in enumerate(units):
            mp[s, u] = tile[:, 256 * k : 256 * (k + 1)].reshape(2, 4, 32, 256)
        for name in ("dx", "ra", "rb", "f", "gr", "gl", "g2", "h", "q"):
            g[n][name] = recv()
        send(mp.at[s, us, oc], dx.at[s, us], partner, dx_out, g[n]["dx"])

    def p1(n):
        s, us, _ = at(n)
        wait(g[n]["dx"], dx.at[s, us])
        mp[s, us, c] += dx[s, us]
        send(mp.at[s, us, c, xo, TOP], ra.at[s, us], x_right, ra_out, g[n]["ra"])
        send(mp.at[s, us, c, xo, LOW], rb.at[s, us], x_left, rb_out, g[n]["rb"])
        send(mp.at[s, us, c, xr, LOW], flr.at[s, us, 0, LOW], x_right, f1_out, g[n]["f"])
        send(mp.at[s, us, c, xl, TOP], flr.at[s, us, 1, TOP], x_left, f1_out, g[n]["f"])

    def p2(n):
        s, us, _ = at(n)
        wait(g[n]["ra"], ra.at[s, us])
        mp[s, us, c, xr, TOP] += ra[s, us]
        send(mp.at[s, us, c, xr, TOP], flr.at[s, us, 0, TOP], x_right, f0_out, g[n]["f"])
        wait(g[n]["rb"], rb.at[s, us])
        mp[s, us, c, xl, LOW] += rb[s, us]
        send(mp.at[s, us, c, xl, LOW], flr.at[s, us, 1, LOW], x_left, f0_out, g[n]["f"])

    def p3(n):
        s, us, _ = at(n)
        wait(g[n]["f"], flr.at[s, us])
        mf[s, us, c, x] = mp[s, us, c, x] + flr[s, us, 0] + flr[s, us, 1]
        top, low, whole = mf.at[s, us, c, x, TOP], mf.at[s, us, c, x, LOW], mf.at[s, us, c, x]
        send(top, top, x_right, g_right, g[n]["gr"])
        send(low, low, x_left, g_left, g[n]["gl"])
        send(low, low, x_right, g_right, g[n]["g2"])
        send(top, top, x_left, g_left, g[n]["g2"])
        send(whole, whole, partner, q_out, g[n]["q"])

    def p4(n):
        s, us, _ = at(n)
        left, right = mf.at[s, us, c, xl], mf.at[s, us, c, xr]
        left_top, right_low = mf.at[s, us, c, xl, TOP], mf.at[s, us, c, xr, LOW]
        wait(g[n]["gr"], left_top)
        send(left_top, left_top, x_right, h_out, g[n]["h"])
        wait(g[n]["gl"], right_low)
        send(right_low, right_low, x_left, h_out, g[n]["h"])
        wait(g[n]["g2"], left)
        send(left, left, partner, q_out, g[n]["q"])
        send(right, right, partner, q_out, g[n]["q"])

    def p5(n):
        s, us, _ = at(n)
        wait(g[n]["h"], mf.at[s, us, c, xo])
        send(mf.at[s, us, c, xo], mf.at[s, us, c, xo], partner, q_out, g[n]["q"])

    begun = set()

    def p6(n, r):
        s, us, units = at(n)
        if "done" not in g[n]:
            wait(g[n]["q"], mf.at[s, us, oc])
            for u in units:
                m_hi[s, u], m_lo[s, u] = split(mf[s, u].reshape(256, 256))
            g[n]["done"] = True
        m = [jnp.concatenate([ref[s, u] for u in units], axis=1) for ref in (m_hi, m_lo)]
        f = [jnp.concatenate([ref[u, r] for u in units], axis=0) for ref in (f_hi, f_lo)]
        part = dot3(*m, *f).reshape(4, 64, 256)
        if (s, r) in begun:
            pacc[s, r] += part
        else:
            pacc[s, r] = part
            begun.add((s, r))

    w = {(s, r): [recv() for _ in range(3)] for s in range(NS) for r in range(2)}
    za_out, zb_out, z1_out, z0_out = sender(za, zb, zlr.at[:, :, 0], zlr.at[:, :, 0])

    def z1(s, r):
        a, b, f = w[s, r]
        send(pacc.at[s, r, 3, LO], za.at[s, r], z_right, za_out, a)
        send(pacc.at[s, r, 3, HI], zb.at[s, r], z_left, zb_out, b)
        send(pacc.at[s, r, 2, HI], zlr.at[s, r, 0, HI], z_right, z1_out, f)
        send(pacc.at[s, r, 1, LO], zlr.at[s, r, 1, LO], z_left, z1_out, f)

    def z2(s, r):
        a, b, f = w[s, r]
        wait(a, za.at[s, r])
        pacc[s, r, 2, LO] += za[s, r]
        send(pacc.at[s, r, 2, LO], zlr.at[s, r, 0, LO], z_right, z0_out, f)
        wait(b, zb.at[s, r])
        pacc[s, r, 1, HI] += zb[s, r]
        send(pacc.at[s, r, 1, HI], zlr.at[s, r, 1, HI], z_left, z0_out, f)

    parity = lax.rem(y, 2)
    t_core = lax.div(y, 2)
    diagonal = x == z

    def t_send_to(s, r, src, to_x, to_z, sem):
        return pltpu.make_async_remote_copy(
            src_ref=src, dst_ref=tb.at[parity, s], send_sem=sem, recv_sem=t_recv.at[s, parity],
            device_id=(to_x, t_core, to_z, 2 * c + r), device_id_type=MESH,
        )

    def t_direct(s, r):
        return t_send_to(s, r, pf.at[s, r], z, x, t_send.at[s, r])

    def t_first(s, r):
        slot, to = (z, dev(z=x)) if RELAY_AXIS == "z" else (x, dev(x=z))
        return pltpu.make_async_remote_copy(
            src_ref=pf.at[s, r], dst_ref=hop.at[s // 2, r, slot], send_sem=t_send.at[s, r],
            recv_sem=hop_recv.at[s // 2, r], device_id=to, device_id_type=MESH,
        )

    def t_second(s, r, d):
        slot = lax.rem(x + d, 4)
        to_x, to_z = (slot, x) if RELAY_AXIS == "z" else (x, slot)
        return t_send_to(s, r, hop.at[s // 2, r, slot], to_x, to_z, hop_send.at[0])

    def mirror(r):
        return jnp.logical_and(jnp.logical_and(diagonal, c == t_core), parity == r)

    def z3(s, r):
        wait(w[s, r][2], zlr.at[s, r])
        pf[s, r] = pacc[s, r, 0] + zlr[s, r, 0] + zlr[s, r, 1]

        @pl.when(mirror(r))
        def _():
            pltpu.make_async_copy(pf.at[s, r], tb.at[parity, s], t_recv.at[s, parity]).start()

        if s in RELAYED:

            @pl.when(jnp.logical_and(diagonal, jnp.logical_not(mirror(r))))
            def _():
                t_direct(s, r).start()

            @pl.when(jnp.logical_not(diagonal))
            def _():
                t_first(s, r).start()

        else:

            @pl.when(jnp.logical_not(mirror(r)))
            def _():
                t_direct(s, r).start()

    def relay(s, r):
        @pl.when(diagonal)
        def _():
            wait(hop_recv.at[s // 2, r], hop.at[0, 0, three])
            for d in range(1, 4):
                t_second(s, r, d).start()

    def t_wait(s, half):
        pltpu.make_async_copy(pf.at[s, 0], tb.at[half, s], t_recv.at[s, half]).wait()

    def history_gram():
        def step(n, acc):
            rows = pl.ds(pl.multiple_of(8 * n, 8), 8)
            acc = list(acc)
            for col in range(2):
                e = [eh[k, rows, lanes[col]] for k in range(6)]
                acc = [v + e[a] * e[b] for v, (a, b) in zip(acc, PAIRS)]
            return tuple(acc)

        acc = lax.fori_loop(0, 64, step, tuple(jnp.zeros((8, 128), F32) for _ in PAIRS))
        return [jnp.sum(v, axis=0, keepdims=True) for v in acc]

    plane, line = 4 * z + y, 2 * x + c
    sum_out = {n: sender(a.at[pl.ds(0, 15)], b.at[pl.ds(0, 7)]) for n, (a, b) in enumerate(((ha, hb), (na, nb)))}
    sum_in = {n: (recv(), recv()) for n in range(2)}

    def sum_plane(n, ref, rows):
        ref[plane] = jnp.concatenate(rows, axis=0)
        for d in range(1, 16):
            to = lax.rem(plane + d, 16)
            send(ref.at[plane], ref.at[plane], dev(z=lax.div(to, 4), y=lax.rem(to, 4)), sum_out[n][0], sum_in[n][0])

    def added(ref, count):
        total = ref[0]
        for k in range(1, count):
            total = total + ref[k]
        return total

    def sum_line(n, ref, before):
        wait(sum_in[n][0], before.at[pl.ds(0, 15)])
        ref[line] = added(before, 16)
        for d in range(1, 8):
            to = lax.rem(line + d, 8)
            send(ref.at[line], ref.at[line], dev(x=lax.div(to, 2), c=lax.rem(to, 2)), sum_out[n][1], sum_in[n][1])

    def sum_end(n, ref):
        wait(sum_in[n][1], ref.at[pl.ds(0, 7)])
        total = jnp.sum(added(ref, 8), axis=1, keepdims=True)
        return jnp.broadcast_to(total, (total.shape[0], 128))

    hist = []

    def first_gram():
        load_e.wait()
        hist.extend(history_gram() + [jnp.zeros((3, 128), F32)])

    def do_ps(s):
        s_line[s].second()
        s_line[s].third()
        prep_s(s, (0, 1, 2, 3))

    def do_pd(u):
        if u == 0:
            for copy in load_d:
                copy.wait()
        if u == 2:
            d_line.second()
        if u == 3:
            d_line.third()
        prep_d(u)

    def do_pf(u, r):
        if u == 0 and r == 0:
            for copy in load_f:
                copy.wait()
        if u == 2:
            f_line[r].second()
        if u == 3:
            f_line[r].third()
        prep_f(u, r)

    work = {
        "ys": lambda _: d_line.begin(), "yf": lambda _: d_line.forward(),
        "fs": lambda r: f_line[r].begin(), "ff": lambda r: f_line[r].forward(),
        "zs": lambda s: s_line[s].begin(), "zf": lambda s: s_line[s].forward(),
        "ps": do_ps, "pd": do_pd, "pf": do_pf, "hist": lambda _: first_gram(),
        "p0": p0, "p1": p1, "p2": p2, "p3": p3, "p4": p4, "p5": p5, "p6": p6,
        "z1": z1, "z2": z2, "z3": z3, "t": relay,
        "ha": lambda: sum_plane(0, ha, hist), "hb": lambda: sum_line(0, hb, ha), "hc": lambda: hist.append(sum_end(0, hb)),
    }
    for phase, *where in ORDER:
        work[phase](*where)

    for n in range(2):
        for r in range(2):
            own[halves[r], lanes[n]] = jnp.concatenate([pf[2 * n, r], pf[2 * n + 1, r]], axis=0).T
    load_h.wait()
    sums = [jnp.zeros((8, 128), F32) for _ in range(7)]
    for s in (1, 0, 2, 3):
        for half in range(2):
            t_wait(s, half)
            start = 256 * half + 64 * s

            def step(n, acc):
                rows = pl.ds(pl.multiple_of(start + 8 * n, 8), 8)
                for col in range(2):
                    e = own[rows, lanes[col]] - tb[half, s, pl.ds(pl.multiple_of(8 * n, 8), 8), lanes[col]]
                    err[rows, lanes[col]] = e
                    acc = tuple(acc[k] + eh[k, rows, lanes[col]] * e for k in range(6)) + (acc[6] + e * e,)
                return acc

            sums = lax.fori_loop(0, 8, step, tuple(sums))
    err_out = load(err, err_hbm)

    sum_plane(1, na, [jnp.sum(v, axis=0, keepdims=True) for v in sums] + [jnp.zeros((1, 128), F32)])
    sum_line(1, nb, na)
    new = sum_end(1, nb)

    gram = {}
    for n, (a, b) in enumerate(PAIRS):
        gram[b, a] = hist[-1][n : n + 1]
    for k in range(7):
        gram[6, k] = new[k : k + 1]
    low = {}
    for j in range(7):
        v = gram[j, j]
        for k in range(j):
            v = v - low[j, k] * low[j, k]
        low[j, j] = jnp.sqrt(v)
        for i in range(j + 1, 7):
            v = gram[i, j]
            for k in range(j):
                v = v - low[i, k] * low[j, k]
            low[i, j] = v / low[j, j]
    forward = []
    for i in range(7):
        v = jnp.ones((1, 128), F32)
        for k in range(i):
            v = v - low[i, k] * forward[k]
        forward.append(v / low[i, i])
    backward = [None] * 7
    for i in range(6, -1, -1):
        v = forward[i]
        for k in range(i + 1, 7):
            v = v - low[k, i] * backward[k]
        backward[i] = v / low[i, i]
    norm = backward[0]
    for v in backward[1:]:
        norm = norm + v
    weights = [v / norm for v in backward]
    lane = lax.broadcasted_iota(jnp.int32, (1, 128), 1)
    row = jnp.zeros((1, 128), F32)
    for k in range(7):
        row = jnp.where(lane == k, weights[k], row)
    w_ref[...] = row
    spread = [jnp.broadcast_to(v, (8, 128)) for v in weights]

    for r in range(2):

        def mix(n, carry):
            part = pl.ds(pl.multiple_of(8 * n, 8), 8)
            rows = pl.ds(pl.multiple_of(256 * r + 8 * n, 8), 8)
            for col in range(2):
                v = spread[6] * fg[0, r, col, part, :]
                for k in range(6):
                    v = v + spread[k] * fh[k, rows, lanes[col]]
                out[rows, lanes[col]] = v
            return carry

        lax.fori_loop(0, 32, mix, 0)
    next_out = load(out, next_hbm)
    for sem, ref in outgoing:
        wait(sem, ref)
    for s in range(NS):
        for r in range(2):

            @pl.when(jnp.logical_not(mirror(r)))
            def _():
                t_direct(s, r).wait_send()

    @pl.when(diagonal)
    def _():
        wait(hop_send.at[0], hop.at[:, :, three])

    err_out.wait()
    next_out.wait()


def body(fock_matrix, density, basis_gram, error_history, fock_history):
    any_ = pl.BlockSpec(memory_space=pl.ANY)
    v = lambda *shape: pltpu.VMEM(shape, F32)
    b = lambda *shape: pltpu.VMEM(shape, BF16)
    dma = pltpu.SemaphoreType.DMA
    block = jax.ShapeDtypeStruct((512, 256), F32)
    next_, err, w = pl.pallas_call(
        kernel,
        out_shape=(block, block, jax.ShapeDtypeStruct((1, 128), F32)),
        in_specs=[any_] * 5,
        out_specs=(any_, any_, pl.BlockSpec(memory_space=pltpu.VMEM)),
        scratch_shapes=[
            v(512, 256), v(4, NS, 64, 512), v(4, 2, 512, 128), v(4, 2, 2, 256, 128),
            b(NS, 256, 512), b(NS, 256, 512), b(NU, 512, 256), b(NU, 512, 256),
            b(NU, 2, 256, 256), b(NU, 2, 256, 256),
            v(NS, NU, 2, 4, 32, 256), v(NS, NU, 4, 32, 256),
            v(NS, NU, 16, 256), v(NS, NU, 16, 256), v(NS, NU, 2, 32, 256),
            v(NS, NU, 2, 4, 32, 256), b(NS, NU, 256, 256), b(NS, NU, 256, 256),
            v(NS, 2, 4, 64, 256), v(NS, 2, 32, 256), v(NS, 2, 32, 256), v(NS, 2, 2, 64, 256),
            v(NS, 2, 64, 256), v(2, NS, 64, 256), v(2, 2, 4, 64, 256),
            v(6, 512, 256), v(6, 512, 256), v(512, 256), v(512, 256), v(512, 256),
            v(16, 24, 128), v(8, 24, 128), v(16, 8, 128), v(8, 8, 128),
            dma((20,)), dma((N_RECV,)), dma((11,)),
            dma((NS, 2)), dma((NS, 2)), dma((2, 2)), dma((1,)),
        ],
        compiler_params=pltpu.CompilerParams(
            collective_id=0, has_side_effects=True, vmem_limit_bytes=60 * 1024 * 1024
        ),
    )(fock_matrix, density, basis_gram, error_history, fock_history)
    return next_, err, w[0, :7]


def solution(mesh):
    split_mesh = Mesh(mesh.devices.reshape(4, 2, 4, 4), ("x", "c", "z", "y"))
    two = P(("x", "c"), ("z", "y"))
    three = P(None, ("x", "c"), ("z", "y"))
    return jax.shard_map(
        body,
        mesh=split_mesh,
        in_specs=(two, two, two, three, three),
        out_specs=(two, two, P()),
        check_vma=False,
    )
```

```python
import jax
import jax.numpy as jnp
from jax import lax
from jax.experimental import pallas as pl
from jax.experimental.pallas import tpu as pltpu
from jax.sharding import Mesh
from jax.sharding import PartitionSpec as P

MESH = pl.DeviceIdType.MESH
F32 = jnp.float32
BF16 = jnp.bfloat16
UNITS = (((0, 0), (0, 1)), ((1, 0), (2, 1)), ((1, 1), (2, 0)), ((3, 0), (3, 1)))
NS, NU = 4, 4
PAIRS = [(a, b) for a in range(6) for b in range(a, 6)]
GROUPS = (
    (0, 0, 1),
    (0, 1, 1),
    (1, 0, 2),
    (0, 2, 1),
    (0, 3, 1),
    (1, 2, 2),
    (2, 0, 2),
    (2, 2, 2),
    (3, 0, 2),
    (3, 2, 1),
    (3, 3, 1),
)
ORDER = (
    ("ys", 0), ("zs", 0), ("hist", 0), ("pd", 0), ("zf", 0), ("zs", 1), ("ps", 0), ("p0", 0), ("zf", 1), ("zs", 2),
    ("yf", 0), ("fs", 0), ("pf", 0, 0), ("pf", 0, 1), ("p1", 0), ("pd", 1), ("p0", 1), ("p1", 1), ("p2", 0),
    ("ps", 1), ("p0", 2), ("zf", 2), ("zs", 3), ("p2", 1), ("pd", 2), ("p0", 3), ("p3", 0), ("p1", 2), ("p1", 3),
    ("p3", 1), ("ps", 2), ("p0", 6), ("p4", 0), ("zf", 3), ("pd", 3), ("p2", 2), ("p0", 4), ("p1", 6), ("p2", 3),
    ("p0", 5), ("p0", 7), ("p5", 0), ("p1", 4), ("p4", 1), ("p1", 5), ("ps", 3), ("ff", 0), ("fs", 1), ("p6", 0, 0),
    ("p2", 6), ("p6", 0, 1), ("pf", 1, 0), ("p0", 8), ("p1", 7), ("p2", 4), ("p0", 9), ("p5", 1), ("pf", 2, 0),
    ("p2", 5), ("p0", 10), ("p3", 2), ("p6", 1, 0), ("p2", 7), ("pf", 3, 0), ("p3", 3), ("p3", 4), ("p3", 5),
    ("p4", 2), ("ff", 1), ("pf", 1, 1), ("p6", 1, 1), ("p1", 8), ("p4", 3), ("p4", 4), ("p3", 6), ("p4", 5),
    ("pf", 2, 1), ("p5", 2), ("p2", 8), ("p6", 2, 0), ("p6", 2, 1), ("p5", 3), ("p5", 4), ("p1", 9), ("pf", 3, 1),
    ("p1", 10), ("p3", 7), ("p6", 3, 0), ("p4", 6), ("p6", 3, 1), ("p5", 5), ("p6", 4, 0), ("z1", 0, 0), ("p6", 4, 1),
    ("z1", 0, 1), ("p2", 9), ("p6", 5, 0), ("z1", 1, 0), ("p2", 10), ("p6", 5, 1), ("p3", 8), ("z1", 1, 1), ("p4", 7),
    ("z2", 0, 0), ("p5", 6), ("p3", 9), ("p3", 10), ("z2", 0, 1), ("p6", 6, 0), ("p6", 6, 1), ("p4", 8), ("z2", 1, 0),
    ("p5", 7), ("p4", 9), ("z2", 1, 1), ("p6", 7, 0), ("z1", 2, 0), ("p4", 10), ("p6", 7, 1), ("z1", 2, 1), ("p5", 8),
    ("z3", 0, 0), ("ha",), ("p5", 9), ("z3", 0, 1), ("z3", 1, 0), ("p6", 8, 0), ("z3", 1, 1), ("p5", 10),
    ("p6", 8, 1), ("z2", 2, 0), ("p6", 9, 0), ("p6", 9, 1), ("p6", 10, 0), ("z1", 3, 0), ("p6", 10, 1), ("z1", 3, 1),
    ("z2", 2, 1), ("z3", 2, 0), ("u", 1), ("z2", 3, 0), ("t", 0, 0), ("t", 0, 1), ("z2", 3, 1), ("z3", 2, 1),
    ("z3", 3, 0), ("z3", 3, 1), ("hb",), ("own",), ("u", 3), ("t", 2, 0), ("t", 2, 1),
)
N_RECV = 49 + 9 * len(GROUPS)
RELAYED = (0, 2)


def split(v):
    hi = v.astype(BF16)
    return hi, (v - hi.astype(F32)).astype(BF16)


def dot3(a_hi, a_lo, b_hi, b_lo):
    a = jnp.concatenate([a_hi, a_hi, a_lo], axis=1)
    b = jnp.concatenate([b_hi, b_lo, b_hi], axis=0)
    return jnp.dot(a, b, preferred_element_type=F32)


def kernel(
    f_hbm, d_hbm, s_hbm, eh_hbm, fh_hbm, out, err, w_ref,
    s_in, sg, dg, fg, s_hi, s_lo, d_hi, d_lo, f_hi, f_lo,
    mp, dx, ra, rb, flr, mf, m_hi, m_lo, pacc, za, zb, zlr, pf, tb, hop, turn,
    eh, fh, own, ha, hb, na, nb,
    send_sem, recv_sem, local_sem, t_send, t_recv, hop_recv, hop_send, turn_recv, turn_send,
):
    x, c, z, y = (lax.axis_index(n) for n in ("x", "c", "z", "y"))
    xr, xl, xo = lax.rem(x + 1, 4), lax.rem(x + 3, 4), lax.rem(x + 2, 4)
    dev = lambda x=x, c=c, z=z, y=y: (x, c, z, y)
    x_right, x_left = dev(x=xr), dev(x=xl)
    d_right, d_left = dev(z=lax.rem(z + 1, 4)), dev(z=lax.rem(z + 3, 4))
    s_right, s_left = dev(y=lax.rem(y + 1, 4)), dev(y=lax.rem(y + 3, 4))
    oc = 1 - c
    partner = dev(c=oc)

    used = {"send": 0, "recv": 0}
    outgoing = []

    def recv():
        used["recv"] += 1
        return recv_sem.at[used["recv"] - 1]

    def sender(*whole):
        used["send"] += len(whole)
        base = used["send"] - len(whole)
        for k, ref in enumerate(whole):
            outgoing.append((send_sem.at[base + k], ref))
        return [send_sem.at[base + k] for k in range(len(whole))]

    def send(src, dst, to, out_sem, in_sem):
        pltpu.make_async_remote_copy(
            src_ref=src, dst_ref=dst, send_sem=out_sem, recv_sem=in_sem, device_id=to, device_id_type=MESH,
        ).start()

    def wait(sem, ref):
        pltpu.make_async_copy(ref, ref, sem).wait()

    local = []

    def load(src, dst):
        copy = pltpu.make_async_copy(src, dst, local_sem.at[len(local)])
        copy.start()
        local.append(copy)
        return copy

    lanes = [pl.ds(0, 128), pl.ds(128, 128)]
    halves = [pl.ds(0, 256), pl.ds(256, 256)]

    barrier = pltpu.get_barrier_semaphore()
    for to in (x_right, x_left, d_right, d_left, s_right, s_left, partner):
        pl.semaphore_signal(barrier, inc=1, device_id=to, device_id_type=MESH)
    load_s = load(s_hbm, s_in)
    load_d = [load(d_hbm.at[:, lanes[h]], dg.at[0, h]) for h in range(2)]
    load_e = load(eh_hbm, eh)
    load_f = [load(f_hbm.at[halves[r], lanes[h]], fg.at[0, r, h]) for r in range(2) for h in range(2)]
    load_h = load(fh_hbm, fh)
    load_s.wait()
    for n in range(2):
        for k in range(4):
            block = s_in[pl.ds(128 * k, 128), lanes[n]].T
            for e in range(2):
                sg[0, 2 * n + e, :, pl.ds(128 * k, 128)] = block[64 * e : 64 * (e + 1)]
    pl.semaphore_wait(barrier, 7)

    three = pl.ds(0, 3)
    (d_out,) = sender(dg.at[three])
    (f_out,) = sender(fg.at[three])
    (s_out,) = sender(sg.at[three])

    class Line:
        def __init__(self, src, slot, size, right, left, out_sem):
            self.src, self.slot, self.size, self.right, self.left, self.out = src, slot, size, right, left, out_sem
            self.sems = [recv() for _ in range(3)]

        def begin(self):
            a, b, _ = self.sems
            send(self.src(0), self.slot(1, 0), self.right, self.out, a)
            send(self.src(1), self.slot(2, 1), self.left, self.out, a)
            send(self.src(1), self.slot(1, 1), self.right, self.out, b)
            send(self.src(0), self.slot(2, 0), self.left, self.out, b)

        def forward(self):
            wait(self.sems[0], self.size)
            send(self.slot(1, 0), self.slot(3, 0), self.right, self.out, self.sems[2])
            send(self.slot(2, 1), self.slot(3, 1), self.left, self.out, self.sems[2])

        def second(self):
            wait(self.sems[1], self.size)

        def third(self):
            wait(self.sems[2], self.size)

    d_line = Line(lambda h: d_hbm.at[:, lanes[h]], lambda slot, h: dg.at[slot, h], dg.at[1], d_right, d_left, d_out)
    f_line = [
        Line(
            lambda h, r=r: f_hbm.at[halves[r], lanes[h]], lambda slot, h, r=r: fg.at[slot, r, h],
            fg.at[1, r], d_right, d_left, f_out,
        )
        for r in range(2)
    ]

    LO, HI = pl.ds(0, 32), pl.ds(32, 32)
    part = (LO, HI)
    s_line = [
        Line(
            lambda h, s=s: sg.at[0, s, part[h]], lambda slot, h, s=s: sg.at[slot, s, part[h]],
            sg.at[1, s], s_right, s_left, s_out,
        )
        for s in range(NS)
    ]

    def prep_s(s, slots):
        for slot in slots:
            hi, lo = split(sg[slot, s])
            at = pl.ds(64 * slot, 64)
            s_hi[s, at, :] = hi
            s_lo[s, at, :] = lo

    def prep_d(u):
        for n, (slot, h) in enumerate(UNITS[u]):
            hi, lo = split(dg[slot, h])
            d_hi[u, :, lanes[n]] = hi
            d_lo[u, :, lanes[n]] = lo

    def prep_f(u, r):
        for n, (slot, h) in enumerate(UNITS[u]):
            for k in range(2):
                hi, lo = split(fg[slot, r, h, lanes[k], :].T)
                f_hi[u, r, lanes[n], lanes[k]] = hi
                f_lo[u, r, lanes[n], lanes[k]] = lo

    TOP, LOW = pl.ds(0, 16), pl.ds(16, 16)
    g = [dict() for _ in GROUPS]

    def at(n):
        s, first, count = GROUPS[n]
        return s, pl.ds(first, count), range(first, first + count)

    dx_out, ra_out, rb_out, f1_out, f0_out, g_right, g_left, h_out, q_out = sender(
        dx, ra, rb, flr.at[:, :, 0], flr.at[:, :, 1], flr.at[:, :, 0], flr.at[:, :, 0], flr.at[:, :, 0], dx
    )

    def p0(n):
        s, us, units = at(n)
        d = [jnp.concatenate([ref[u] for u in units], axis=1) for ref in (d_hi, d_lo)]
        tile = dot3(s_hi[s], s_lo[s], *d)
        for k, u in enumerate(units):
            mp[s, u] = tile[:, 256 * k : 256 * (k + 1)].reshape(2, 4, 32, 256)
        for name in ("dx", "ra", "rb", "f", "gr", "gl", "g2", "h", "q"):
            g[n][name] = recv()
        send(mp.at[s, us, oc], dx.at[s, us], partner, dx_out, g[n]["dx"])

    def p1(n):
        s, us, _ = at(n)
        wait(g[n]["dx"], dx.at[s, us])
        mp[s, us, c] += dx[s, us]
        send(mp.at[s, us, c, xo, TOP], ra.at[s, us], x_right, ra_out, g[n]["ra"])
        send(mp.at[s, us, c, xo, LOW], rb.at[s, us], x_left, rb_out, g[n]["rb"])
        send(mp.at[s, us, c, xr, LOW], flr.at[s, us, 0, LOW], x_right, f1_out, g[n]["f"])
        send(mp.at[s, us, c, xl, TOP], flr.at[s, us, 1, TOP], x_left, f1_out, g[n]["f"])

    def p2(n):
        s, us, _ = at(n)
        wait(g[n]["ra"], ra.at[s, us])
        mp[s, us, c, xr, TOP] += ra[s, us]
        send(mp.at[s, us, c, xr, TOP], flr.at[s, us, 0, TOP], x_right, f0_out, g[n]["f"])
        wait(g[n]["rb"], rb.at[s, us])
        mp[s, us, c, xl, LOW] += rb[s, us]
        send(mp.at[s, us, c, xl, LOW], flr.at[s, us, 1, LOW], x_left, f0_out, g[n]["f"])

    def p3(n):
        s, us, _ = at(n)
        wait(g[n]["f"], flr.at[s, us])
        mf[s, us, c, x] = mp[s, us, c, x] + flr[s, us, 0] + flr[s, us, 1]
        top, low, whole = mf.at[s, us, c, x, TOP], mf.at[s, us, c, x, LOW], mf.at[s, us, c, x]
        send(top, top, x_right, g_right, g[n]["gr"])
        send(low, low, x_left, g_left, g[n]["gl"])
        send(low, low, x_right, g_right, g[n]["g2"])
        send(top, top, x_left, g_left, g[n]["g2"])
        send(whole, whole, partner, q_out, g[n]["q"])

    def p4(n):
        s, us, _ = at(n)
        left, right = mf.at[s, us, c, xl], mf.at[s, us, c, xr]
        left_top, right_low = mf.at[s, us, c, xl, TOP], mf.at[s, us, c, xr, LOW]
        wait(g[n]["gr"], left_top)
        send(left_top, left_top, x_right, h_out, g[n]["h"])
        wait(g[n]["gl"], right_low)
        send(right_low, right_low, x_left, h_out, g[n]["h"])
        wait(g[n]["g2"], left)
        send(left, left, partner, q_out, g[n]["q"])
        send(right, right, partner, q_out, g[n]["q"])

    def p5(n):
        s, us, _ = at(n)
        wait(g[n]["h"], mf.at[s, us, c, xo])
        send(mf.at[s, us, c, xo], mf.at[s, us, c, xo], partner, q_out, g[n]["q"])

    begun = set()

    def p6(n, r):
        s, us, units = at(n)
        if "done" not in g[n]:
            wait(g[n]["q"], mf.at[s, us, oc])
            for u in units:
                m_hi[s, u], m_lo[s, u] = split(mf[s, u].reshape(256, 256))
            g[n]["done"] = True
        m = [jnp.concatenate([ref[s, u] for u in units], axis=1) for ref in (m_hi, m_lo)]
        f = [jnp.concatenate([ref[u, r] for u in units], axis=0) for ref in (f_hi, f_lo)]
        part = dot3(*m, *f).reshape(4, 64, 256)
        if (s, r) in begun:
            pacc[s, r] += part
        else:
            pacc[s, r] = part
            begun.add((s, r))

    w = {(s, r): [recv() for _ in range(3)] for s in range(NS) for r in range(2)}
    za_out, zb_out, z1_out, z0_out = sender(za, zb, zlr.at[:, :, 0], zlr.at[:, :, 0])

    def z1(s, r):
        a, b, f = w[s, r]
        send(pacc.at[s, r, 3, LO], za.at[s, r], s_right, za_out, a)
        send(pacc.at[s, r, 3, HI], zb.at[s, r], s_left, zb_out, b)
        send(pacc.at[s, r, 2, HI], zlr.at[s, r, 0, HI], s_right, z1_out, f)
        send(pacc.at[s, r, 1, LO], zlr.at[s, r, 1, LO], s_left, z1_out, f)

    def z2(s, r):
        a, b, f = w[s, r]
        wait(a, za.at[s, r])
        pacc[s, r, 2, LO] += za[s, r]
        send(pacc.at[s, r, 2, LO], zlr.at[s, r, 0, LO], s_right, z0_out, f)
        wait(b, zb.at[s, r])
        pacc[s, r, 1, HI] += zb[s, r]
        send(pacc.at[s, r, 1, HI], zlr.at[s, r, 1, HI], s_left, z0_out, f)

    parity = lax.rem(y, 2)
    t_core = lax.div(y, 2)
    diagonal = x == z
    stays = [jnp.logical_and(c == t_core, parity == r) for r in range(2)]

    def t_send_to(s, r, src, to_x, to_z, sem):
        return pltpu.make_async_remote_copy(
            src_ref=src, dst_ref=tb.at[s, parity], send_sem=sem, recv_sem=t_recv.at[s],
            device_id=(to_x, t_core, to_z, 2 * c + r), device_id_type=MESH,
        )

    def t_first(s, r):
        src = pf.at[s, r]
        yield diagonal, stays[r], tb.at[s, parity], t_recv.at[s], (x, t_core, z, 2 * c + r)
        if s in RELAYED:
            k = RELAYED.index(s)
            yield jnp.logical_not(diagonal), None, hop.at[k, r, z], hop_recv.at[k, r], dev(z=x)
        else:
            k = s // 2
            yield jnp.logical_not(diagonal), stays[r], turn.at[k, parity], turn_recv.at[k], (x, t_core, z, 2 * c + r)

    def t_copy(s, r, dst, sem, to):
        return pltpu.make_async_remote_copy(
            src_ref=pf.at[s, r], dst_ref=dst, send_sem=t_send.at[s, r], recv_sem=sem, device_id=to, device_id_type=MESH,
        )

    def t_second(s, r, d):
        slot = lax.rem(x + d, 4)
        return t_send_to(s, r, hop.at[RELAYED.index(s), r, slot], slot, x, hop_send.at[0])

    def turned(s):
        return pltpu.make_async_remote_copy(
            src_ref=turn.at[s // 2], dst_ref=tb.at[s], send_sem=turn_send.at[0], recv_sem=t_recv.at[s],
            device_id=dev(x=z, z=x), device_id_type=MESH,
        )

    def z3(s, r):
        wait(w[s, r][2], zlr.at[s, r])
        pf[s, r] = pacc[s, r, 0] + zlr[s, r, 0] + zlr[s, r, 1]
        for case, local_case, dst, sem, to in t_first(s, r):
            away = case if local_case is None else jnp.logical_and(case, jnp.logical_not(local_case))

            @pl.when(away)
            def _(dst=dst, sem=sem, to=to):
                t_copy(s, r, dst, sem, to).start()

            if local_case is not None:

                @pl.when(jnp.logical_and(case, local_case))
                def _(dst=dst, sem=sem):
                    pltpu.make_async_copy(pf.at[s, r], dst, sem).start()

    def pass_on(s):
        @pl.when(jnp.logical_not(diagonal))
        def _():
            wait(turn_recv.at[s // 2], turn.at[s // 2])
            turned(s).start()

    def relay(s, r):
        @pl.when(diagonal)
        def _():
            wait(hop_recv.at[RELAYED.index(s), r], hop.at[0, 0, three])
            for d in range(1, 4):
                t_second(s, r, d).start()

    def turn_own():
        for n in range(2):
            for r in range(2):
                own[halves[r], lanes[n]] = jnp.concatenate([pf[2 * n, r], pf[2 * n + 1, r]], axis=0).T

    def history_gram():
        def step(n, acc):
            rows = pl.ds(pl.multiple_of(8 * n, 8), 8)
            acc = list(acc)
            for col in range(2):
                e = [eh[k, rows, lanes[col]] for k in range(6)]
                acc = [v + e[a] * e[b] for v, (a, b) in zip(acc, PAIRS)]
            return tuple(acc)

        acc = lax.fori_loop(0, 64, step, tuple(jnp.zeros((8, 128), F32) for _ in PAIRS))
        return [jnp.sum(v, axis=0, keepdims=True) for v in acc]

    plane, line = 4 * z + y, 2 * x + c
    sum_out = {n: sender(a.at[pl.ds(0, 15)], b.at[pl.ds(0, 7)]) for n, (a, b) in enumerate(((ha, hb), (na, nb)))}
    sum_in = {n: (recv(), recv()) for n in range(2)}

    def sum_plane(n, ref, rows):
        ref[plane] = jnp.concatenate(rows, axis=0)
        for d in range(1, 16):
            to = lax.rem(plane + d, 16)
            send(ref.at[plane], ref.at[plane], dev(z=lax.div(to, 4), y=lax.rem(to, 4)), sum_out[n][0], sum_in[n][0])

    def added(ref, count):
        total = ref[0]
        for k in range(1, count):
            total = total + ref[k]
        return total

    def sum_line(n, ref, before):
        wait(sum_in[n][0], before.at[pl.ds(0, 15)])
        ref[line] = added(before, 16)
        for d in range(1, 8):
            to = lax.rem(line + d, 8)
            send(ref.at[line], ref.at[line], dev(x=lax.div(to, 2), c=lax.rem(to, 2)), sum_out[n][1], sum_in[n][1])

    def sum_end(n, ref):
        wait(sum_in[n][1], ref.at[pl.ds(0, 7)])
        total = jnp.sum(added(ref, 8), axis=1, keepdims=True)
        return jnp.broadcast_to(total, (total.shape[0], 128))

    hist = []

    def first_gram():
        load_e.wait()
        hist.extend(history_gram() + [jnp.zeros((3, 128), F32)])

    def do_ps(s):
        s_line[s].second()
        s_line[s].third()
        prep_s(s, (0, 1, 2, 3))

    def do_pd(u):
        if u == 0:
            for copy in load_d:
                copy.wait()
        if u == 2:
            d_line.second()
        if u == 3:
            d_line.third()
        prep_d(u)

    def do_pf(u, r):
        if u == 0 and r == 0:
            for copy in load_f:
                copy.wait()
        if u == 2:
            f_line[r].second()
        if u == 3:
            f_line[r].third()
        prep_f(u, r)

    work = {
        "ys": lambda _: d_line.begin(), "yf": lambda _: d_line.forward(),
        "fs": lambda r: f_line[r].begin(), "ff": lambda r: f_line[r].forward(),
        "zs": lambda s: s_line[s].begin(), "zf": lambda s: s_line[s].forward(),
        "ps": do_ps, "pd": do_pd, "pf": do_pf, "hist": lambda _: first_gram(),
        "p0": p0, "p1": p1, "p2": p2, "p3": p3, "p4": p4, "p5": p5, "p6": p6,
        "z1": z1, "z2": z2, "z3": z3, "t": relay, "u": pass_on, "own": turn_own,
        "ha": lambda: sum_plane(0, ha, hist), "hb": lambda: sum_line(0, hb, ha),
    }
    for phase, *where in ORDER:
        work[phase](*where)

    load_h.wait()
    sums = [jnp.zeros((8, 128), F32) for _ in range(7)]
    for s in (1, 0, 3, 2):
        wait(t_recv.at[s], tb.at[s])
        for half in range(2):
            start = 256 * half + 64 * s

            def step(n, acc):
                rows = pl.ds(pl.multiple_of(start + 8 * n, 8), 8)
                for col in range(2):
                    e = own[rows, lanes[col]] - tb[s, half, pl.ds(pl.multiple_of(8 * n, 8), 8), lanes[col]]
                    err[rows, lanes[col]] = e
                    acc = tuple(acc[k] + eh[k, rows, lanes[col]] * e for k in range(6)) + (acc[6] + e * e,)
                return acc

            sums = lax.fori_loop(0, 8, step, tuple(sums))

    sum_plane(1, na, [jnp.sum(v, axis=0, keepdims=True) for v in sums] + [jnp.zeros((1, 128), F32)])
    sum_line(1, nb, na)
    hist.append(sum_end(0, hb))
    new = sum_end(1, nb)

    gram = {}
    for n, (a, b) in enumerate(PAIRS):
        gram[b, a] = hist[-1][n : n + 1]
    for k in range(7):
        gram[6, k] = new[k : k + 1]
    low = {}
    for j in range(7):
        v = gram[j, j]
        for k in range(j):
            v = v - low[j, k] * low[j, k]
        low[j, j] = jnp.sqrt(v)
        for i in range(j + 1, 7):
            v = gram[i, j]
            for k in range(j):
                v = v - low[i, k] * low[j, k]
            low[i, j] = v / low[j, j]
    forward = []
    for i in range(7):
        v = jnp.ones((1, 128), F32)
        for k in range(i):
            v = v - low[i, k] * forward[k]
        forward.append(v / low[i, i])
    backward = [None] * 7
    for i in range(6, -1, -1):
        v = forward[i]
        for k in range(i + 1, 7):
            v = v - low[k, i] * backward[k]
        backward[i] = v / low[i, i]
    norm = backward[0]
    for v in backward[1:]:
        norm = norm + v
    weights = [v / norm for v in backward]
    lane = lax.broadcasted_iota(jnp.int32, (1, 128), 1)
    row = jnp.zeros((1, 128), F32)
    for k in range(7):
        row = jnp.where(lane == k, weights[k], row)
    w_ref[...] = row
    spread = [jnp.broadcast_to(v, (8, 128)) for v in weights]

    for r in range(2):

        def mix(n, carry):
            part = pl.ds(pl.multiple_of(8 * n, 8), 8)
            rows = pl.ds(pl.multiple_of(256 * r + 8 * n, 8), 8)
            for col in range(2):
                v = spread[6] * fg[0, r, col, part, :]
                for k in range(6):
                    v = v + spread[k] * fh[k, rows, lanes[col]]
                out[rows, lanes[col]] = v
            return carry

        lax.fori_loop(0, 32, mix, 0)
    for sem, ref in outgoing:
        wait(sem, ref)
    for s in range(NS):
        for r in range(2):
            here = jnp.logical_and(diagonal, stays[r]) if s in RELAYED else stays[r]

            @pl.when(jnp.logical_not(here))
            def _():
                wait(t_send.at[s, r], pf.at[s, r])

    @pl.when(jnp.logical_not(diagonal))
    def _():
        wait(turn_send.at[0], turn)

    @pl.when(diagonal)
    def _():
        wait(hop_send.at[0], hop.at[:, :, three])


def body(fock_matrix, density, basis_gram, error_history, fock_history):
    any_ = pl.BlockSpec(memory_space=pl.ANY)
    v = lambda *shape: pltpu.VMEM(shape, F32)
    b = lambda *shape: pltpu.VMEM(shape, BF16)
    dma = pltpu.SemaphoreType.DMA
    block = pltpu.VMEM((512, 256), F32)
    next_, err, w = pl.pallas_call(
        kernel,
        out_shape=(block, block, pltpu.VMEM((1, 128), F32)),
        in_specs=[any_] * 5,
        out_specs=(pl.BlockSpec(memory_space=pltpu.VMEM),) * 3,
        scratch_shapes=[
            v(512, 256), v(4, NS, 64, 512), v(4, 2, 512, 128), v(4, 2, 2, 256, 128),
            b(NS, 256, 512), b(NS, 256, 512), b(NU, 512, 256), b(NU, 512, 256),
            b(NU, 2, 256, 256), b(NU, 2, 256, 256),
            v(NS, NU, 2, 4, 32, 256), v(NS, NU, 4, 32, 256),
            v(NS, NU, 16, 256), v(NS, NU, 16, 256), v(NS, NU, 2, 32, 256),
            v(NS, NU, 2, 4, 32, 256), b(NS, NU, 256, 256), b(NS, NU, 256, 256),
            v(NS, 2, 4, 64, 256), v(NS, 2, 32, 256), v(NS, 2, 32, 256), v(NS, 2, 2, 64, 256),
            v(NS, 2, 64, 256), v(NS, 2, 64, 256), v(2, 2, 4, 64, 256), v(2, 2, 64, 256),
            v(6, 512, 256), v(6, 512, 256), v(512, 256),
            v(16, 24, 128), v(8, 24, 128), v(16, 8, 128), v(8, 8, 128),
            dma((20,)), dma((N_RECV,)), dma((9,)),
            dma((NS, 2)), dma((NS,)), dma((2, 2)), dma((1,)), dma((2,)), dma((1,)),
        ],
        compiler_params=pltpu.CompilerParams(
            collective_id=0, has_side_effects=True, vmem_limit_bytes=60 * 1024 * 1024
        ),
    )(fock_matrix, density, basis_gram, error_history, fock_history)
    return next_, err, w[0, :7]


def solution(mesh):
    split_mesh = Mesh(mesh.devices.reshape(4, 2, 4, 4), ("x", "c", "z", "y"))
    two = P(("x", "c"), ("z", "y"))
    three = P(None, ("x", "c"), ("z", "y"))
    return jax.shard_map(
        body,
        mesh=split_mesh,
        in_specs=(two, two, two, three, three),
        out_specs=(two, two, P()),
        check_vma=False,
    )
```

```python
import jax
import jax.numpy as jnp
from jax import lax
from jax.experimental import pallas as pl
from jax.experimental.pallas import tpu as pltpu
from jax.sharding import Mesh
from jax.sharding import PartitionSpec as P

MESH = pl.DeviceIdType.MESH
F32 = jnp.float32
BF16 = jnp.bfloat16
UNITS = (((0, 0), (0, 1)), ((1, 0), (2, 1)), ((1, 1), (2, 0)), ((3, 0), (3, 1)))
NS, NU = 4, 4
PAIRS = [(a, b) for a in range(6) for b in range(a, 6)]
GROUPS = (
    (0, 0, 1), (0, 1, 1), (1, 0, 2), (0, 2, 1), (0, 3, 1), (1, 2, 2), (2, 0, 2), (2, 2, 2), (3, 0, 2), (3, 2, 1),
    (3, 3, 1),
)
ORDER = (
    ("ys", 0), ("zs", 0), ("zs", 1), ("zf", 0), ("zf", 1), ("zs", 3), ("yf", 0), ("pd", 0), ("zs", 2), ("fs", 0),
    ("pd", 1), ("ps", 0), ("p0", 1), ("p0", 0), ("ps", 1), ("p0", 2), ("p1", 1), ("p1", 0), ("p1", 2), ("hist", 0),
    ("zf", 3), ("p2", 1), ("pd", 2), ("p2", 0), ("p0", 3), ("zf", 2), ("p2", 2), ("p1", 3), ("p3", 1), ("p3", 0),
    ("p3", 2), ("pd", 3), ("p0", 4), ("p0", 5), ("p2", 3), ("p4", 1), ("p1", 4), ("ps", 2), ("p4", 0), ("ps", 3),
    ("pf", 0, 0), ("p1", 5), ("p0", 7), ("ff", 0), ("p3", 3), ("p2", 4), ("p1", 7), ("p0", 6), ("fs", 1), ("p2", 5),
    ("p4", 2), ("p4", 3), ("p3", 4), ("p0", 10), ("p5", 0), ("p1", 6), ("p0", 9), ("p5", 1), ("pf", 1, 0), ("p3", 5),
    ("p6", 1, 0), ("p0", 8), ("p4", 4), ("p1", 9), ("p2", 7), ("p5", 3), ("ff", 1), ("pf", 0, 1), ("pf", 1, 1),
    ("pf", 3, 0), ("p6", 0, 0), ("p1", 10), ("p2", 6), ("pf", 2, 0), ("p4", 5), ("p5", 2), ("p1", 8), ("p5", 4),
    ("p6", 3, 0), ("p6", 4, 0), ("z1", 0, 0), ("p6", 0, 1), ("pf", 2, 1), ("p3", 7), ("p6", 1, 1), ("p2", 9),
    ("p6", 3, 1), ("pf", 3, 1), ("p6", 4, 1), ("z1", 0, 1), ("p3", 6), ("p5", 5), ("p2", 10), ("p6", 2, 0),
    ("p6", 2, 1), ("z2", 0, 0), ("p6", 5, 0), ("z1", 1, 0), ("p2", 8), ("p4", 7), ("p3", 9), ("z2", 0, 1),
    ("p6", 5, 1), ("z1", 1, 1), ("p4", 6), ("p3", 10), ("z2", 1, 0), ("p3", 8), ("z3", 0, 0), ("p5", 7), ("z3", 0, 1),
    ("ha",), ("p4", 9), ("z2", 1, 1), ("p5", 6), ("p6", 7, 0), ("p6", 7, 1), ("p4", 10), ("z3", 1, 0), ("p6", 6, 0),
    ("p6", 6, 1), ("p4", 8), ("z1", 2, 1), ("p5", 9), ("z3", 1, 1), ("z1", 2, 0), ("p5", 10), ("p6", 9, 0), ("p5", 8),
    ("p6", 10, 0), ("z2", 2, 1), ("p6", 10, 1), ("p6", 8, 0), ("z1", 3, 0), ("p6", 9, 1), ("u", 1), ("z2", 2, 0),
    ("p6", 8, 1), ("z1", 3, 1), ("t", 1, 1), ("u", 0), ("z2", 3, 0), ("z3", 2, 1), ("t", 0, 1), ("z2", 3, 1),
    ("t", 1, 0), ("z3", 2, 0), ("z3", 3, 0), ("t", 0, 0), ("z3", 3, 1), ("own",), ("t", 2, 1), ("t", 2, 0), ("u", 2),
    ("t", 3, 0), ("t", 3, 1), ("hb",),
)
N_RECV = 41 + 7 * len(GROUPS)
TURNED = 3


def split(v):
    hi = v.astype(BF16)
    return hi, (v - hi.astype(F32)).astype(BF16)


def dot3(a_hi, a_lo, b_hi, b_lo):
    a = jnp.concatenate([a_hi, a_hi, a_lo], axis=1)
    b = jnp.concatenate([b_hi, b_lo, b_hi], axis=0)
    return jnp.dot(a, b, preferred_element_type=F32)


def kernel(
    f_hbm, d_hbm, s_hbm, eh_hbm, fh_hbm, out, err, w_ref,
    s_in, sg, dg, fg, s_hi, s_lo, d_hi, d_lo, f_hi, f_lo,
    mp, dx, rab, flr, mf, m_hi, m_lo, pacc, zab, zlr, pf, tb, hop, turn,
    eh, fh, own, ha, hb, na, nb,
    send_sem, recv_sem, local_sem, t_send, t_recv, hop_recv, hop_send, turn_recv, turn_send,
):
    x, c, z, y = (lax.axis_index(n) for n in ("x", "c", "z", "y"))
    xr, xl, xo = lax.rem(x + 1, 4), lax.rem(x + 3, 4), lax.rem(x + 2, 4)
    dev = lambda x=x, c=c, z=z, y=y: (x, c, z, y)
    x_right, x_left = dev(x=xr), dev(x=xl)
    d_right, d_left = dev(z=lax.rem(z + 1, 4)), dev(z=lax.rem(z + 3, 4))
    s_right, s_left = dev(y=lax.rem(y + 1, 4)), dev(y=lax.rem(y + 3, 4))
    oc = 1 - c
    partner = dev(c=oc)

    used = {"send": 0, "recv": 0}
    outgoing = []

    def recv():
        used["recv"] += 1
        return recv_sem.at[used["recv"] - 1]

    def sender(*whole):
        used["send"] += len(whole)
        base = used["send"] - len(whole)
        for k, ref in enumerate(whole):
            outgoing.append((send_sem.at[base + k], ref))
        return [send_sem.at[base + k] for k in range(len(whole))]

    def send(src, dst, to, out_sem, in_sem):
        pltpu.make_async_remote_copy(
            src_ref=src, dst_ref=dst, send_sem=out_sem, recv_sem=in_sem, device_id=to, device_id_type=MESH,
        ).start()

    def wait(sem, ref):
        pltpu.make_async_copy(ref, ref, sem).wait()

    local = []

    def load(src, dst):
        copy = pltpu.make_async_copy(src, dst, local_sem.at[len(local)])
        copy.start()
        local.append(copy)
        return copy

    lanes = [pl.ds(0, 128), pl.ds(128, 128)]
    halves = [pl.ds(0, 256), pl.ds(256, 256)]

    barrier = pltpu.get_barrier_semaphore()
    for to in (x_right, x_left, d_right, d_left, s_right, s_left, partner):
        pl.semaphore_signal(barrier, inc=1, device_id=to, device_id_type=MESH)
    load_s = load(s_hbm, s_in)
    load_d = [load(d_hbm.at[:, lanes[h]], dg.at[0, h]) for h in range(2)]
    load_e = load(eh_hbm, eh)
    load_f = [load(f_hbm.at[halves[r], lanes[h]], fg.at[0, r, h]) for r in range(2) for h in range(2)]
    load_h = load(fh_hbm, fh)
    load_s.wait()
    for n in range(2):
        for k in range(4):
            block = s_in[pl.ds(128 * k, 128), lanes[n]].T
            for e in range(2):
                sg[0, 2 * n + e, :, pl.ds(128 * k, 128)] = block[64 * e : 64 * (e + 1)]
    pl.semaphore_wait(barrier, 7)

    three = pl.ds(0, 3)
    (d_out,) = sender(dg.at[three])
    (f_out,) = sender(fg.at[three])
    (s_out,) = sender(sg.at[three])

    class Line:
        def __init__(self, src, slot, size, right, left, out_sem):
            self.src, self.slot, self.size, self.right, self.left, self.out = src, slot, size, right, left, out_sem
            self.sems = [recv() for _ in range(3)]

        def begin(self):
            a, b, _ = self.sems
            send(self.src(0), self.slot(1, 0), self.right, self.out, a)
            send(self.src(1), self.slot(2, 1), self.left, self.out, a)
            send(self.src(1), self.slot(1, 1), self.right, self.out, b)
            send(self.src(0), self.slot(2, 0), self.left, self.out, b)

        def forward(self):
            wait(self.sems[0], self.size)
            send(self.slot(1, 0), self.slot(3, 0), self.right, self.out, self.sems[2])
            send(self.slot(2, 1), self.slot(3, 1), self.left, self.out, self.sems[2])

        def second(self):
            wait(self.sems[1], self.size)

        def third(self):
            wait(self.sems[2], self.size)

    d_line = Line(lambda h: d_hbm.at[:, lanes[h]], lambda slot, h: dg.at[slot, h], dg.at[1], d_right, d_left, d_out)
    f_line = [
        Line(
            lambda h, r=r: f_hbm.at[halves[r], lanes[h]], lambda slot, h, r=r: fg.at[slot, r, h],
            fg.at[1, r], d_right, d_left, f_out,
        )
        for r in range(2)
    ]

    LO, HI = pl.ds(0, 32), pl.ds(32, 32)
    part = (LO, HI)
    s_line = [
        Line(
            lambda h, s=s: sg.at[0, s, part[h]], lambda slot, h, s=s: sg.at[slot, s, part[h]],
            sg.at[1, s], s_right, s_left, s_out,
        )
        for s in range(NS)
    ]

    def prep_s(s, slots):
        for slot in slots:
            hi, lo = split(sg[slot, s])
            at = pl.ds(64 * slot, 64)
            s_hi[s, at, :] = hi
            s_lo[s, at, :] = lo

    def prep_d(u):
        for n, (slot, h) in enumerate(UNITS[u]):
            hi, lo = split(dg[slot, h])
            d_hi[u, :, lanes[n]] = hi
            d_lo[u, :, lanes[n]] = lo

    def prep_f(u, r):
        for n, (slot, h) in enumerate(UNITS[u]):
            for k in range(2):
                hi, lo = split(fg[slot, r, h, lanes[k], :].T)
                f_hi[u, r, lanes[n], lanes[k]] = hi
                f_lo[u, r, lanes[n], lanes[k]] = lo

    TOP, LOW = pl.ds(0, 16), pl.ds(16, 16)
    g = [dict() for _ in GROUPS]

    def at(n):
        s, first, count = GROUPS[n]
        return s, pl.ds(first, count), range(first, first + count)

    dx_out, r_out, f1_out, f0_out, g_right, g_left, h_out, q_out = sender(
        dx, rab, flr.at[:, :, 0], flr.at[:, :, 1], flr.at[:, :, 0], flr.at[:, :, 0], flr.at[:, :, 0], dx
    )

    def p0(n):
        s, us, units = at(n)
        d = [jnp.concatenate([ref[u] for u in units], axis=1) for ref in (d_hi, d_lo)]
        tile = dot3(s_hi[s], s_lo[s], *d)
        for k, u in enumerate(units):
            mp[s, u] = tile[:, 256 * k : 256 * (k + 1)].reshape(2, 4, 32, 256)
        for name in ("dx", "r", "f", "g1", "g2", "h", "q"):
            g[n][name] = recv()
        send(mp.at[s, us, oc], dx.at[s, us], partner, dx_out, g[n]["dx"])

    def p1(n):
        s, us, _ = at(n)
        wait(g[n]["dx"], dx.at[s, us])
        mp[s, us, c] += dx[s, us]
        send(mp.at[s, us, c, xo, TOP], rab.at[s, us, 0], x_right, r_out, g[n]["r"])
        send(mp.at[s, us, c, xo, LOW], rab.at[s, us, 1], x_left, r_out, g[n]["r"])
        send(mp.at[s, us, c, xr, LOW], flr.at[s, us, 0, LOW], x_right, f1_out, g[n]["f"])
        send(mp.at[s, us, c, xl, TOP], flr.at[s, us, 1, TOP], x_left, f1_out, g[n]["f"])

    def p2(n):
        s, us, _ = at(n)
        wait(g[n]["r"], rab.at[s, us])
        mp[s, us, c, xr, TOP] += rab[s, us, 0]
        send(mp.at[s, us, c, xr, TOP], flr.at[s, us, 0, TOP], x_right, f0_out, g[n]["f"])
        mp[s, us, c, xl, LOW] += rab[s, us, 1]
        send(mp.at[s, us, c, xl, LOW], flr.at[s, us, 1, LOW], x_left, f0_out, g[n]["f"])

    def p3(n):
        s, us, _ = at(n)
        wait(g[n]["f"], flr.at[s, us])
        mf[s, us, c, x] = mp[s, us, c, x] + flr[s, us, 0] + flr[s, us, 1]
        top, low, whole = mf.at[s, us, c, x, TOP], mf.at[s, us, c, x, LOW], mf.at[s, us, c, x]
        send(top, top, x_right, g_right, g[n]["g1"])
        send(low, low, x_left, g_left, g[n]["g1"])
        send(low, low, x_right, g_right, g[n]["g2"])
        send(top, top, x_left, g_left, g[n]["g2"])
        send(whole, whole, partner, q_out, g[n]["q"])

    def p4(n):
        s, us, _ = at(n)
        left, right = mf.at[s, us, c, xl], mf.at[s, us, c, xr]
        left_top, right_low = mf.at[s, us, c, xl, TOP], mf.at[s, us, c, xr, LOW]
        wait(g[n]["g1"], left)
        send(left_top, left_top, x_right, h_out, g[n]["h"])
        send(right_low, right_low, x_left, h_out, g[n]["h"])
        wait(g[n]["g2"], left)
        send(left, left, partner, q_out, g[n]["q"])
        send(right, right, partner, q_out, g[n]["q"])

    def p5(n):
        s, us, _ = at(n)
        wait(g[n]["h"], mf.at[s, us, c, xo])
        send(mf.at[s, us, c, xo], mf.at[s, us, c, xo], partner, q_out, g[n]["q"])

    begun = set()

    def p6(n, r):
        s, us, units = at(n)
        if "done" not in g[n]:
            wait(g[n]["q"], mf.at[s, us, oc])
            for u in units:
                m_hi[s, u], m_lo[s, u] = split(mf[s, u].reshape(256, 256))
            g[n]["done"] = True
        m = [jnp.concatenate([ref[s, u] for u in units], axis=1) for ref in (m_hi, m_lo)]
        f = [jnp.concatenate([ref[u, r] for u in units], axis=0) for ref in (f_hi, f_lo)]
        part = dot3(*m, *f).reshape(4, 64, 256)
        if (s, r) in begun:
            pacc[s, r] += part
        else:
            pacc[s, r] = part
            begun.add((s, r))

    w = {(s, r): (recv(), recv()) for s in range(NS) for r in range(2)}
    za_out, z1_out, z0_out = sender(zab, zlr.at[:, :, 0], zlr.at[:, :, 0])

    def z1(s, r):
        a, f = w[s, r]
        send(pacc.at[s, r, 3, LO], zab.at[s, r, 0], s_right, za_out, a)
        send(pacc.at[s, r, 3, HI], zab.at[s, r, 1], s_left, za_out, a)
        send(pacc.at[s, r, 2, HI], zlr.at[s, r, 0, HI], s_right, z1_out, f)
        send(pacc.at[s, r, 1, LO], zlr.at[s, r, 1, LO], s_left, z1_out, f)

    def z2(s, r):
        a, f = w[s, r]
        wait(a, zab.at[s, r])
        pacc[s, r, 2, LO] += zab[s, r, 0]
        send(pacc.at[s, r, 2, LO], zlr.at[s, r, 0, LO], s_right, z0_out, f)
        pacc[s, r, 1, HI] += zab[s, r, 1]
        send(pacc.at[s, r, 1, HI], zlr.at[s, r, 1, HI], s_left, z0_out, f)

    parity = lax.rem(y, 2)
    t_core = lax.div(y, 2)
    apart = lax.rem(x - z + 4, 4)
    diagonal, far = apart == 0, apart == 2
    near = jnp.logical_or(apart == 1, apart == 3)
    stays = [jnp.logical_and(c == t_core, parity == r) for r in range(2)]

    def t_first(s, r):
        end, in_plane = (tb.at[s, parity], t_recv.at[s]), (x, t_core, z, 2 * c + r)
        yield diagonal, stays[r], *end, in_plane
        yield far, None, hop.at[s, r], hop_recv.at[s, r], dev(z=x)
        if s < TURNED:
            yield near, stays[r], turn.at[s, parity], turn_recv.at[s], in_plane
        else:
            yield near, None, *end, (z, t_core, x, 2 * c + r)

    def t_copy(s, r, dst, sem, to):
        return pltpu.make_async_remote_copy(
            src_ref=pf.at[s, r], dst_ref=dst, send_sem=t_send.at[s, r], recv_sem=sem, device_id=to, device_id_type=MESH,
        )

    def z3(s, r):
        wait(w[s, r][1], zlr.at[s, r])
        pf[s, r] = pacc[s, r, 0] + zlr[s, r, 0] + zlr[s, r, 1]
        for case, local_case, dst, sem, to in t_first(s, r):
            away = case if local_case is None else jnp.logical_and(case, jnp.logical_not(local_case))

            @pl.when(away)
            def _(dst=dst, sem=sem, to=to):
                t_copy(s, r, dst, sem, to).start()

            if local_case is not None:

                @pl.when(jnp.logical_and(case, local_case))
                def _(dst=dst, sem=sem):
                    pltpu.make_async_copy(pf.at[s, r], dst, sem).start()

    def pass_on(s):
        @pl.when(near)
        def _():
            wait(turn_recv.at[s], turn.at[s])
            send(turn.at[s], tb.at[s], dev(x=z, z=x), turn_send.at[0], t_recv.at[s])

    def relay(s, r):
        @pl.when(diagonal)
        def _():
            wait(hop_recv.at[s, r], hop.at[s, r])
            send(hop.at[s, r], tb.at[s, parity], (xo, t_core, x, 2 * c + r), hop_send.at[0], t_recv.at[s])

    def turn_own():
        for n in range(2):
            for r in range(2):
                own[halves[r], lanes[n]] = jnp.concatenate([pf[2 * n, r], pf[2 * n + 1, r]], axis=0).T

    def history_gram():
        def step(n, acc):
            rows = pl.ds(pl.multiple_of(8 * n, 8), 8)
            acc = list(acc)
            for col in range(2):
                e = [eh[k, rows, lanes[col]] for k in range(6)]
                acc = [v + e[a] * e[b] for v, (a, b) in zip(acc, PAIRS)]
            return tuple(acc)

        acc = lax.fori_loop(0, 64, step, tuple(jnp.zeros((8, 128), F32) for _ in PAIRS))
        return [jnp.sum(v, axis=0, keepdims=True) for v in acc]

    plane, line = 4 * z + y, 2 * x + c
    sum_out = {n: sender(a.at[pl.ds(0, 15)], b.at[pl.ds(0, 7)]) for n, (a, b) in enumerate(((ha, hb), (na, nb)))}
    sum_in = {n: (recv(), recv()) for n in range(2)}

    def sum_plane(n, ref, rows):
        ref[plane] = jnp.concatenate(rows, axis=0)
        for d in range(1, 16):
            to = lax.rem(plane + d, 16)
            send(ref.at[plane], ref.at[plane], dev(z=lax.div(to, 4), y=lax.rem(to, 4)), sum_out[n][0], sum_in[n][0])

    def added(ref, count):
        total = ref[0]
        for k in range(1, count):
            total = total + ref[k]
        return total

    def sum_line(n, ref, before):
        wait(sum_in[n][0], before.at[pl.ds(0, 15)])
        ref[line] = added(before, 16)
        for d in range(1, 8):
            to = lax.rem(line + d, 8)
            send(ref.at[line], ref.at[line], dev(x=lax.div(to, 2), c=lax.rem(to, 2)), sum_out[n][1], sum_in[n][1])

    def sum_end(n, ref):
        wait(sum_in[n][1], ref.at[pl.ds(0, 7)])
        total = jnp.sum(added(ref, 8), axis=1, keepdims=True)
        return jnp.broadcast_to(total, (total.shape[0], 128))

    hist = []

    def first_gram():
        load_e.wait()
        hist.extend(history_gram() + [jnp.zeros((3, 128), F32)])

    def do_ps(s):
        s_line[s].second()
        s_line[s].third()
        prep_s(s, (0, 1, 2, 3))

    def do_pd(u):
        if u == 0:
            for copy in load_d:
                copy.wait()
        if u == 2:
            d_line.second()
        if u == 3:
            d_line.third()
        prep_d(u)

    def do_pf(u, r):
        if u == 0 and r == 0:
            for copy in load_f:
                copy.wait()
        if u == 2:
            f_line[r].second()
        if u == 3:
            f_line[r].third()
        prep_f(u, r)

    work = {
        "ys": lambda _: d_line.begin(), "yf": lambda _: d_line.forward(),
        "fs": lambda r: f_line[r].begin(), "ff": lambda r: f_line[r].forward(),
        "zs": lambda s: s_line[s].begin(), "zf": lambda s: s_line[s].forward(),
        "ps": do_ps, "pd": do_pd, "pf": do_pf, "hist": lambda _: first_gram(),
        "p0": p0, "p1": p1, "p2": p2, "p3": p3, "p4": p4, "p5": p5, "p6": p6,
        "z1": z1, "z2": z2, "z3": z3, "t": relay, "u": pass_on, "own": turn_own,
        "ha": lambda: sum_plane(0, ha, hist), "hb": lambda: sum_line(0, hb, ha),
    }
    for phase, *where in ORDER:
        work[phase](*where)

    load_h.wait()
    sums = [jnp.zeros((8, 128), F32) for _ in range(7)]
    for s in range(NS):
        wait(t_recv.at[s], tb.at[s])
        for half in range(2):
            start = 256 * half + 64 * s

            def step(n, acc):
                rows = pl.ds(pl.multiple_of(start + 8 * n, 8), 8)
                for col in range(2):
                    e = own[rows, lanes[col]] - tb[s, half, pl.ds(pl.multiple_of(8 * n, 8), 8), lanes[col]]
                    err[rows, lanes[col]] = e
                    acc = tuple(acc[k] + eh[k, rows, lanes[col]] * e for k in range(6)) + (acc[6] + e * e,)
                return acc

            sums = lax.fori_loop(0, 8, step, tuple(sums))

    sum_plane(1, na, [jnp.sum(v, axis=0, keepdims=True) for v in sums] + [jnp.zeros((1, 128), F32)])
    sum_line(1, nb, na)
    hist.append(sum_end(0, hb))
    new = sum_end(1, nb)

    gram = {}
    for n, (a, b) in enumerate(PAIRS):
        gram[b, a] = hist[-1][n : n + 1]
    for k in range(7):
        gram[6, k] = new[k : k + 1]
    low = {}
    for j in range(7):
        v = gram[j, j]
        for k in range(j):
            v = v - low[j, k] * low[j, k]
        low[j, j] = jnp.sqrt(v)
        for i in range(j + 1, 7):
            v = gram[i, j]
            for k in range(j):
                v = v - low[i, k] * low[j, k]
            low[i, j] = v / low[j, j]
    forward = []
    for i in range(7):
        v = jnp.ones((1, 128), F32)
        for k in range(i):
            v = v - low[i, k] * forward[k]
        forward.append(v / low[i, i])
    backward = [None] * 7
    for i in range(6, -1, -1):
        v = forward[i]
        for k in range(i + 1, 7):
            v = v - low[k, i] * backward[k]
        backward[i] = v / low[i, i]
    norm = backward[0]
    for v in backward[1:]:
        norm = norm + v
    weights = [v / norm for v in backward]
    lane = lax.broadcasted_iota(jnp.int32, (1, 128), 1)
    row = jnp.zeros((1, 128), F32)
    for k in range(7):
        row = jnp.where(lane == k, weights[k], row)
    w_ref[...] = row

    for r in range(2):

        def mix(n, carry):
            part = pl.ds(pl.multiple_of(32 * n, 32), 32)
            rows = pl.ds(pl.multiple_of(256 * r + 32 * n, 32), 32)
            for col in range(2):
                v = weights[6] * fg[0, r, col, part, :]
                for k in range(6):
                    v = v + weights[k] * fh[k, rows, lanes[col]]
                out[rows, lanes[col]] = v
            return carry

        lax.fori_loop(0, 8, mix, 0)
    for sem, ref in outgoing:
        wait(sem, ref)
    for s in range(NS):
        for r in range(2):
            here = jnp.logical_and(stays[r], jnp.logical_or(diagonal, near) if s < TURNED else diagonal)

            @pl.when(jnp.logical_not(here))
            def _():
                wait(t_send.at[s, r], pf.at[s, r])

    @pl.when(near)
    def _():
        wait(turn_send.at[0], turn)

    @pl.when(diagonal)
    def _():
        wait(hop_send.at[0], hop)


def body(fock_matrix, density, basis_gram, error_history, fock_history):
    any_ = pl.BlockSpec(memory_space=pl.ANY)
    v = lambda *shape: pltpu.VMEM(shape, F32)
    b = lambda *shape: pltpu.VMEM(shape, BF16)
    dma = pltpu.SemaphoreType.DMA
    block = pltpu.VMEM((512, 256), F32)
    next_, err, w = pl.pallas_call(
        kernel,
        out_shape=(block, block, pltpu.VMEM((1, 128), F32)),
        in_specs=[any_] * 5,
        out_specs=(pl.BlockSpec(memory_space=pltpu.VMEM),) * 3,
        scratch_shapes=[
            v(512, 256), v(4, NS, 64, 512), v(4, 2, 512, 128), v(4, 2, 2, 256, 128),
            b(NS, 256, 512), b(NS, 256, 512), b(NU, 512, 256), b(NU, 512, 256),
            b(NU, 2, 256, 256), b(NU, 2, 256, 256),
            v(NS, NU, 2, 4, 32, 256), v(NS, NU, 4, 32, 256),
            v(NS, NU, 2, 16, 256), v(NS, NU, 2, 32, 256),
            v(NS, NU, 2, 4, 32, 256), b(NS, NU, 256, 256), b(NS, NU, 256, 256),
            v(NS, 2, 4, 64, 256), v(NS, 2, 2, 32, 256), v(NS, 2, 2, 64, 256),
            v(NS, 2, 64, 256), v(NS, 2, 64, 256), v(NS, 2, 64, 256), v(TURNED, 2, 64, 256),
            v(6, 512, 256), v(6, 512, 256), v(512, 256),
            v(16, 24, 128), v(8, 24, 128), v(16, 8, 128), v(8, 8, 128),
            dma((18,)), dma((N_RECV,)), dma((9,)),
            dma((NS, 2)), dma((NS,)), dma((NS, 2)), dma((1,)), dma((TURNED,)), dma((1,)),
        ],
        compiler_params=pltpu.CompilerParams(
            collective_id=0, has_side_effects=True, vmem_limit_bytes=60 * 1024 * 1024
        ),
    )(fock_matrix, density, basis_gram, error_history, fock_history)
    return next_, err, w[0, :7]


def solution(mesh):
    split_mesh = Mesh(mesh.devices.reshape(4, 2, 4, 4), ("x", "c", "z", "y"))
    two = P(("x", "c"), ("z", "y"))
    three = P(None, ("x", "c"), ("z", "y"))
    return jax.shard_map(
        body,
        mesh=split_mesh,
        in_specs=(two, two, two, three, three),
        out_specs=(two, two, P()),
        check_vma=False,
    )
```

```python
import jax
import jax.numpy as jnp
from jax import lax
from jax.experimental import pallas as pl
from jax.experimental.pallas import tpu as pltpu
from jax.sharding import Mesh
from jax.sharding import PartitionSpec as P

MESH = pl.DeviceIdType.MESH
F32 = jnp.float32
BF16 = jnp.bfloat16
UNITS = (((0, 0), (0, 1)), ((1, 0), (2, 1)), ((1, 1), (2, 0)), ((3, 0), (3, 1)))
NS, NU = 4, 4
PAIRS = [(a, b) for a in range(6) for b in range(a, 6)]
GROUPS = (
    (0, 0, 1), (0, 1, 1), (1, 0, 2), (0, 2, 1), (0, 3, 1), (1, 2, 2), (2, 0, 2), (2, 2, 2), (3, 0, 2), (3, 2, 1),
    (3, 3, 1),
)
ORDER = (
    ("ys", 0), ("zs", 1), ("zs", 0), ("zf", 1), ("zf", 0), ("yf", 0), ("pd", 1), ("pd", 0), ("ps", 1), ("p0", 2),
    ("zs", 2), ("ps", 0), ("p0", 0), ("fs", 0), ("p1", 2), ("p1", 0), ("p0", 1), ("p2", 2), ("pd", 2), ("zf", 2),
    ("p1", 1), ("p0", 3), ("p2", 0), ("p1", 3), ("p3", 2), ("p2", 1), ("pd", 3), ("p3", 0), ("p0", 4), ("p0", 5),
    ("p2", 3), ("zs", 3), ("p1", 4), ("ps", 2), ("p1", 5), ("p0", 7), ("ff", 0), ("p3", 1), ("pf", 1, 0), ("p3", 3),
    ("p2", 4), ("zf", 3), ("p2", 5), ("p4", 0), ("fs", 1), ("p4", 2), ("hist", 0), ("pf", 2, 0), ("p4", 1), ("p0", 6),
    ("p4", 3), ("pf", 0, 0), ("p3", 4), ("p1", 7), ("ps", 3), ("p0", 8), ("p0", 9), ("p5", 2), ("p5", 0), ("p3", 5),
    ("p0", 10), ("pf", 0, 1), ("p4", 4), ("p5", 1), ("p1", 6), ("p6", 2, 0), ("p5", 3), ("pf", 3, 0), ("ff", 1),
    ("p6", 0, 0), ("pf", 1, 1), ("p2", 7), ("p6", 1, 0), ("p6", 3, 0), ("p6", 2, 1), ("p4", 5), ("p5", 4), ("p1", 8),
    ("pf", 2, 1), ("p6", 4, 0), ("p2", 6), ("z1", 0, 0), ("p6", 0, 1), ("p1", 9), ("p6", 3, 1), ("p6", 1, 1),
    ("p1", 10), ("pf", 3, 1), ("p5", 5), ("p6", 4, 1), ("z1", 0, 1), ("p3", 7), ("p6", 5, 0), ("z1", 1, 0), ("p3", 6),
    ("z2", 0, 0), ("p2", 9), ("p2", 8), ("z2", 0, 1), ("p2", 10), ("p6", 5, 1), ("z1", 1, 1), ("p4", 7), ("z2", 1, 0),
    ("p4", 6), ("z3", 0, 0), ("p3", 9), ("z3", 0, 1), ("ha",), ("p3", 8), ("p5", 7), ("p3", 10), ("z2", 1, 1),
    ("p5", 6), ("z3", 1, 0), ("p6", 7, 0), ("p4", 9), ("p6", 6, 0), ("z1", 2, 0), ("p6", 6, 1), ("p4", 8),
    ("p6", 7, 1), ("z1", 2, 1), ("p4", 10), ("p5", 9), ("z3", 1, 1), ("p5", 8), ("t", 0, 1), ("p6", 9, 0), ("p5", 10),
    ("z2", 2, 0), ("z2", 2, 1), ("p6", 8, 0), ("p6", 10, 0), ("z1", 3, 0), ("p6", 9, 1), ("p6", 8, 1), ("p6", 10, 1),
    ("z1", 3, 1), ("t", 0, 0), ("z2", 3, 0), ("t", 1, 1), ("z3", 2, 0), ("z2", 3, 1), ("z3", 2, 1), ("u", 1),
    ("z3", 3, 0), ("t", 1, 0), ("z3", 3, 1), ("own",), ("t", 2, 0), ("u", 0), ("t", 2, 1), ("t", 3, 0),
    ("t", 3, 1), ("hb",),
)
N_RECV = 41 + 7 * len(GROUPS)
TURNED = 2


def split(v):
    hi = v.astype(BF16)
    return hi, (v - hi.astype(F32)).astype(BF16)


def dot3(a_hi, a_lo, b_hi, b_lo):
    a = jnp.concatenate([a_hi, a_hi, a_lo], axis=1)
    b = jnp.concatenate([b_hi, b_lo, b_hi], axis=0)
    return jnp.dot(a, b, preferred_element_type=F32)


def kernel(
    f_hbm, d_hbm, s_hbm, eh_hbm, fh_hbm, out, err, w_ref,
    s_in, sg, dg, fg, s_hi, s_lo, d_hi, d_lo, f_hi, f_lo,
    mp, dx, rab, flr, mf, m_hi, m_lo, pacc, zab, zlr, pf, tb, hop, turn,
    eh, fh, own, ha, hb, na, nb,
    send_sem, recv_sem, local_sem, t_send, t_recv, hop_recv, hop_send, turn_recv, turn_send,
):
    x, c, z, y = (lax.axis_index(n) for n in ("x", "c", "z", "y"))
    xr, xl, xo = lax.rem(x + 1, 4), lax.rem(x + 3, 4), lax.rem(x + 2, 4)
    dev = lambda x=x, c=c, z=z, y=y: (x, c, z, y)
    x_right, x_left = dev(x=xr), dev(x=xl)
    d_right, d_left = dev(z=lax.rem(z + 1, 4)), dev(z=lax.rem(z + 3, 4))
    s_right, s_left = dev(y=lax.rem(y + 1, 4)), dev(y=lax.rem(y + 3, 4))
    oc = 1 - c
    partner = dev(c=oc)

    used = {"send": 0, "recv": 0}
    outgoing = []

    def recv():
        used["recv"] += 1
        return recv_sem.at[used["recv"] - 1]

    def sender(*whole):
        used["send"] += len(whole)
        base = used["send"] - len(whole)
        for k, ref in enumerate(whole):
            outgoing.append((send_sem.at[base + k], ref))
        return [send_sem.at[base + k] for k in range(len(whole))]

    def send(src, dst, to, out_sem, in_sem):
        pltpu.make_async_remote_copy(
            src_ref=src, dst_ref=dst, send_sem=out_sem, recv_sem=in_sem, device_id=to, device_id_type=MESH,
        ).start()

    def wait(sem, ref):
        pltpu.make_async_copy(ref, ref, sem).wait()

    local = []

    def load(src, dst):
        copy = pltpu.make_async_copy(src, dst, local_sem.at[len(local)])
        copy.start()
        local.append(copy)
        return copy

    lanes = [pl.ds(0, 128), pl.ds(128, 128)]
    halves = [pl.ds(0, 256), pl.ds(256, 256)]

    barrier = pltpu.get_barrier_semaphore()
    for to in (x_right, x_left, d_right, d_left, s_right, s_left, partner):
        pl.semaphore_signal(barrier, inc=1, device_id=to, device_id_type=MESH)
    load_s = load(s_hbm, s_in)
    load_d = [load(d_hbm.at[:, lanes[h]], dg.at[0, h]) for h in range(2)]
    load_e = load(eh_hbm, eh)
    load_f = [load(f_hbm.at[halves[r], lanes[h]], fg.at[0, r, h]) for r in range(2) for h in range(2)]
    load_h = load(fh_hbm, fh)
    load_s.wait()
    for n in range(2):
        for k in range(4):
            block = s_in[pl.ds(128 * k, 128), lanes[n]].T
            for e in range(2):
                sg[0, 2 * n + e, :, pl.ds(128 * k, 128)] = block[64 * e : 64 * (e + 1)]
    pl.semaphore_wait(barrier, 7)

    three = pl.ds(0, 3)
    (d_out,) = sender(dg.at[three])
    (f_out,) = sender(fg.at[three])
    (s_out,) = sender(sg.at[three])

    class Line:
        def __init__(self, src, slot, size, right, left, out_sem):
            self.src, self.slot, self.size, self.right, self.left, self.out = src, slot, size, right, left, out_sem
            self.sems = [recv() for _ in range(3)]

        def begin(self):
            a, b, _ = self.sems
            send(self.src(0), self.slot(1, 0), self.right, self.out, a)
            send(self.src(1), self.slot(2, 1), self.left, self.out, a)
            send(self.src(1), self.slot(1, 1), self.right, self.out, b)
            send(self.src(0), self.slot(2, 0), self.left, self.out, b)

        def forward(self):
            wait(self.sems[0], self.size)
            send(self.slot(1, 0), self.slot(3, 0), self.right, self.out, self.sems[2])
            send(self.slot(2, 1), self.slot(3, 1), self.left, self.out, self.sems[2])

        def second(self):
            wait(self.sems[1], self.size)

        def third(self):
            wait(self.sems[2], self.size)

    d_line = Line(lambda h: d_hbm.at[:, lanes[h]], lambda slot, h: dg.at[slot, h], dg.at[1], d_right, d_left, d_out)
    f_line = [
        Line(
            lambda h, r=r: f_hbm.at[halves[r], lanes[h]], lambda slot, h, r=r: fg.at[slot, r, h],
            fg.at[1, r], d_right, d_left, f_out,
        )
        for r in range(2)
    ]

    LO, HI = pl.ds(0, 32), pl.ds(32, 32)
    part = (LO, HI)
    s_line = [
        Line(
            lambda h, s=s: sg.at[0, s, part[h]], lambda slot, h, s=s: sg.at[slot, s, part[h]],
            sg.at[1, s], s_right, s_left, s_out,
        )
        for s in range(NS)
    ]

    def prep_s(s, slots):
        for slot in slots:
            hi, lo = split(sg[slot, s])
            at = pl.ds(64 * slot, 64)
            s_hi[s, at, :] = hi
            s_lo[s, at, :] = lo

    def prep_d(u):
        for n, (slot, h) in enumerate(UNITS[u]):
            hi, lo = split(dg[slot, h])
            d_hi[u, :, lanes[n]] = hi
            d_lo[u, :, lanes[n]] = lo

    def prep_f(u, r):
        for n, (slot, h) in enumerate(UNITS[u]):
            for k in range(2):
                hi, lo = split(fg[slot, r, h, lanes[k], :].T)
                f_hi[u, r, lanes[n], lanes[k]] = hi
                f_lo[u, r, lanes[n], lanes[k]] = lo

    TOP, LOW = pl.ds(0, 16), pl.ds(16, 16)
    g = [dict() for _ in GROUPS]

    def at(n):
        s, first, count = GROUPS[n]
        return s, pl.ds(first, count), range(first, first + count)

    dx_out, r_out, f1_out, f0_out, g_right, g_left, h_out, q_out = sender(
        dx, rab, flr.at[:, :, 0], flr.at[:, :, 1], flr.at[:, :, 0], flr.at[:, :, 0], flr.at[:, :, 0], dx
    )

    def p0(n):
        s, us, units = at(n)
        d = [jnp.concatenate([ref[u] for u in units], axis=1) for ref in (d_hi, d_lo)]
        tile = dot3(s_hi[s], s_lo[s], *d)
        for k, u in enumerate(units):
            mp[s, u] = tile[:, 256 * k : 256 * (k + 1)].reshape(2, 4, 32, 256)
        for name in ("dx", "r", "f", "g1", "g2", "h", "q"):
            g[n][name] = recv()
        send(mp.at[s, us, oc], dx.at[s, us], partner, dx_out, g[n]["dx"])

    def p1(n):
        s, us, _ = at(n)
        wait(g[n]["dx"], dx.at[s, us])
        mp[s, us, c] += dx[s, us]
        send(mp.at[s, us, c, xo, TOP], rab.at[s, us, 0], x_right, r_out, g[n]["r"])
        send(mp.at[s, us, c, xo, LOW], rab.at[s, us, 1], x_left, r_out, g[n]["r"])
        send(mp.at[s, us, c, xr, LOW], flr.at[s, us, 0, LOW], x_right, f1_out, g[n]["f"])
        send(mp.at[s, us, c, xl, TOP], flr.at[s, us, 1, TOP], x_left, f1_out, g[n]["f"])

    def p2(n):
        s, us, _ = at(n)
        wait(g[n]["r"], rab.at[s, us])
        mp[s, us, c, xr, TOP] += rab[s, us, 0]
        send(mp.at[s, us, c, xr, TOP], flr.at[s, us, 0, TOP], x_right, f0_out, g[n]["f"])
        mp[s, us, c, xl, LOW] += rab[s, us, 1]
        send(mp.at[s, us, c, xl, LOW], flr.at[s, us, 1, LOW], x_left, f0_out, g[n]["f"])

    def p3(n):
        s, us, _ = at(n)
        wait(g[n]["f"], flr.at[s, us])
        mf[s, us, c, x] = mp[s, us, c, x] + flr[s, us, 0] + flr[s, us, 1]
        top, low, whole = mf.at[s, us, c, x, TOP], mf.at[s, us, c, x, LOW], mf.at[s, us, c, x]
        send(top, top, x_right, g_right, g[n]["g1"])
        send(low, low, x_left, g_left, g[n]["g1"])
        send(low, low, x_right, g_right, g[n]["g2"])
        send(top, top, x_left, g_left, g[n]["g2"])
        send(whole, whole, partner, q_out, g[n]["q"])

    def p4(n):
        s, us, _ = at(n)
        left, right = mf.at[s, us, c, xl], mf.at[s, us, c, xr]
        left_top, right_low = mf.at[s, us, c, xl, TOP], mf.at[s, us, c, xr, LOW]
        wait(g[n]["g1"], left)
        send(left_top, left_top, x_right, h_out, g[n]["h"])
        send(right_low, right_low, x_left, h_out, g[n]["h"])
        wait(g[n]["g2"], left)
        send(left, left, partner, q_out, g[n]["q"])
        send(right, right, partner, q_out, g[n]["q"])

    def p5(n):
        s, us, _ = at(n)
        wait(g[n]["h"], mf.at[s, us, c, xo])
        send(mf.at[s, us, c, xo], mf.at[s, us, c, xo], partner, q_out, g[n]["q"])

    begun = set()

    def p6(n, r):
        s, us, units = at(n)
        if "done" not in g[n]:
            wait(g[n]["q"], mf.at[s, us, oc])
            for u in units:
                m_hi[s, u], m_lo[s, u] = split(mf[s, u].reshape(256, 256))
            g[n]["done"] = True
        m = [jnp.concatenate([ref[s, u] for u in units], axis=1) for ref in (m_hi, m_lo)]
        f = [jnp.concatenate([ref[u, r] for u in units], axis=0) for ref in (f_hi, f_lo)]
        part = dot3(*m, *f).reshape(4, 64, 256)
        if (s, r) in begun:
            pacc[s, r] += part
        else:
            pacc[s, r] = part
            begun.add((s, r))

    w = {(s, r): (recv(), recv()) for s in range(NS) for r in range(2)}
    za_out, z1_out, z0_out = sender(zab, zlr.at[:, :, 0], zlr.at[:, :, 0])

    def z1(s, r):
        a, f = w[s, r]
        send(pacc.at[s, r, 3, LO], zab.at[s, r, 0], s_right, za_out, a)
        send(pacc.at[s, r, 3, HI], zab.at[s, r, 1], s_left, za_out, a)
        send(pacc.at[s, r, 2, HI], zlr.at[s, r, 0, HI], s_right, z1_out, f)
        send(pacc.at[s, r, 1, LO], zlr.at[s, r, 1, LO], s_left, z1_out, f)

    def z2(s, r):
        a, f = w[s, r]
        wait(a, zab.at[s, r])
        pacc[s, r, 2, LO] += zab[s, r, 0]
        send(pacc.at[s, r, 2, LO], zlr.at[s, r, 0, LO], s_right, z0_out, f)
        pacc[s, r, 1, HI] += zab[s, r, 1]
        send(pacc.at[s, r, 1, HI], zlr.at[s, r, 1, HI], s_left, z0_out, f)

    parity = lax.rem(y, 2)
    t_core = lax.div(y, 2)
    apart = lax.rem(x - z + 4, 4)
    diagonal, far = apart == 0, apart == 2
    near = jnp.logical_or(apart == 1, apart == 3)
    stays = [jnp.logical_and(c == t_core, parity == r) for r in range(2)]

    def t_first(s, r):
        end, in_plane = (tb.at[s, parity], t_recv.at[s]), (x, t_core, z, 2 * c + r)
        yield diagonal, stays[r], *end, in_plane
        yield far, None, hop.at[s, r], hop_recv.at[s, r], dev(z=x)
        if s < TURNED:
            yield near, stays[r], turn.at[s, parity], turn_recv.at[s], in_plane
        else:
            yield near, None, *end, (z, t_core, x, 2 * c + r)

    def t_copy(s, r, dst, sem, to):
        return pltpu.make_async_remote_copy(
            src_ref=pf.at[s, r], dst_ref=dst, send_sem=t_send.at[s, r], recv_sem=sem, device_id=to, device_id_type=MESH,
        )

    def z3(s, r):
        wait(w[s, r][1], zlr.at[s, r])
        pf[s, r] = pacc[s, r, 0] + zlr[s, r, 0] + zlr[s, r, 1]
        for case, local_case, dst, sem, to in t_first(s, r):
            away = case if local_case is None else jnp.logical_and(case, jnp.logical_not(local_case))

            @pl.when(away)
            def _(dst=dst, sem=sem, to=to):
                t_copy(s, r, dst, sem, to).start()

            if local_case is not None:

                @pl.when(jnp.logical_and(case, local_case))
                def _(dst=dst, sem=sem):
                    pltpu.make_async_copy(pf.at[s, r], dst, sem).start()

    def pass_on(s):
        @pl.when(near)
        def _():
            wait(turn_recv.at[s], turn.at[s])
            send(turn.at[s], tb.at[s], dev(x=z, z=x), turn_send.at[0], t_recv.at[s])

    def relay(s, r):
        @pl.when(diagonal)
        def _():
            wait(hop_recv.at[s, r], hop.at[s, r])
            send(hop.at[s, r], tb.at[s, parity], (xo, t_core, x, 2 * c + r), hop_send.at[0], t_recv.at[s])

    def turn_own():
        for n in range(2):
            for r in range(2):
                own[halves[r], lanes[n]] = jnp.concatenate([pf[2 * n, r], pf[2 * n + 1, r]], axis=0).T

    def history_gram():
        def step(n, acc):
            rows = pl.ds(pl.multiple_of(8 * n, 8), 8)
            acc = list(acc)
            for col in range(2):
                e = [eh[k, rows, lanes[col]] for k in range(6)]
                acc = [v + e[a] * e[b] for v, (a, b) in zip(acc, PAIRS)]
            return tuple(acc)

        acc = lax.fori_loop(0, 64, step, tuple(jnp.zeros((8, 128), F32) for _ in PAIRS))
        return [jnp.sum(v, axis=0, keepdims=True) for v in acc]

    plane, line = 4 * z + y, 2 * x + c
    sum_out = {n: sender(a.at[pl.ds(0, 15)], b.at[pl.ds(0, 7)]) for n, (a, b) in enumerate(((ha, hb), (na, nb)))}
    sum_in = {n: (recv(), recv()) for n in range(2)}

    def sum_plane(n, ref, rows):
        ref[plane] = jnp.concatenate(rows, axis=0)
        for d in range(1, 16):
            to = lax.rem(plane + d, 16)
            send(ref.at[plane], ref.at[plane], dev(z=lax.div(to, 4), y=lax.rem(to, 4)), sum_out[n][0], sum_in[n][0])

    def added(ref, count):
        total = ref[0]
        for k in range(1, count):
            total = total + ref[k]
        return total

    def sum_line(n, ref, before):
        wait(sum_in[n][0], before.at[pl.ds(0, 15)])
        ref[line] = added(before, 16)
        for d in range(1, 8):
            to = lax.rem(line + d, 8)
            send(ref.at[line], ref.at[line], dev(x=lax.div(to, 2), c=lax.rem(to, 2)), sum_out[n][1], sum_in[n][1])

    def sum_end(n, ref):
        wait(sum_in[n][1], ref.at[pl.ds(0, 7)])
        total = jnp.sum(added(ref, 8), axis=1, keepdims=True)
        return jnp.broadcast_to(total, (total.shape[0], 128))

    hist = []

    def first_gram():
        load_e.wait()
        hist.extend(history_gram() + [jnp.zeros((3, 128), F32)])

    def do_ps(s):
        s_line[s].second()
        s_line[s].third()
        prep_s(s, (0, 1, 2, 3))

    def do_pd(u):
        if u == 0:
            for copy in load_d:
                copy.wait()
        if u == 2:
            d_line.second()
        if u == 3:
            d_line.third()
        prep_d(u)

    def do_pf(u, r):
        if u == 0 and r == 0:
            for copy in load_f:
                copy.wait()
        if u == 2:
            f_line[r].second()
        if u == 3:
            f_line[r].third()
        prep_f(u, r)

    work = {
        "ys": lambda _: d_line.begin(), "yf": lambda _: d_line.forward(),
        "fs": lambda r: f_line[r].begin(), "ff": lambda r: f_line[r].forward(),
        "zs": lambda s: s_line[s].begin(), "zf": lambda s: s_line[s].forward(),
        "ps": do_ps, "pd": do_pd, "pf": do_pf, "hist": lambda _: first_gram(),
        "p0": p0, "p1": p1, "p2": p2, "p3": p3, "p4": p4, "p5": p5, "p6": p6,
        "z1": z1, "z2": z2, "z3": z3, "t": relay, "u": pass_on, "own": turn_own,
        "ha": lambda: sum_plane(0, ha, hist), "hb": lambda: sum_line(0, hb, ha),
    }
    for phase, *where in ORDER:
        work[phase](*where)

    load_h.wait()
    sums = [jnp.zeros((8, 128), F32) for _ in range(7)]
    for s in range(NS):
        wait(t_recv.at[s], tb.at[s])
        for half in range(2):
            start = 256 * half + 64 * s

            def step(n, acc):
                rows = pl.ds(pl.multiple_of(start + 8 * n, 8), 8)
                for col in range(2):
                    e = own[rows, lanes[col]] - tb[s, half, pl.ds(pl.multiple_of(8 * n, 8), 8), lanes[col]]
                    err[rows, lanes[col]] = e
                    acc = tuple(acc[k] + eh[k, rows, lanes[col]] * e for k in range(6)) + (acc[6] + e * e,)
                return acc

            sums = lax.fori_loop(0, 8, step, tuple(sums))

    sum_plane(1, na, [jnp.sum(v, axis=0, keepdims=True) for v in sums] + [jnp.zeros((1, 128), F32)])
    sum_line(1, nb, na)
    hist.append(sum_end(0, hb))
    new = sum_end(1, nb)

    gram = {}
    for n, (a, b) in enumerate(PAIRS):
        gram[b, a] = hist[-1][n : n + 1]
    for k in range(7):
        gram[6, k] = new[k : k + 1]
    low = {}
    for j in range(7):
        v = gram[j, j]
        for k in range(j):
            v = v - low[j, k] * low[j, k]
        low[j, j] = jnp.sqrt(v)
        for i in range(j + 1, 7):
            v = gram[i, j]
            for k in range(j):
                v = v - low[i, k] * low[j, k]
            low[i, j] = v / low[j, j]
    forward = []
    for i in range(7):
        v = jnp.ones((1, 128), F32)
        for k in range(i):
            v = v - low[i, k] * forward[k]
        forward.append(v / low[i, i])
    backward = [None] * 7
    for i in range(6, -1, -1):
        v = forward[i]
        for k in range(i + 1, 7):
            v = v - low[k, i] * backward[k]
        backward[i] = v / low[i, i]
    norm = backward[0]
    for v in backward[1:]:
        norm = norm + v
    weights = [v / norm for v in backward]
    lane = lax.broadcasted_iota(jnp.int32, (1, 128), 1)
    row = jnp.zeros((1, 128), F32)
    for k in range(7):
        row = jnp.where(lane == k, weights[k], row)
    w_ref[...] = row

    for r in range(2):

        def mix(n, carry):
            part = pl.ds(pl.multiple_of(32 * n, 32), 32)
            rows = pl.ds(pl.multiple_of(256 * r + 32 * n, 32), 32)
            for col in range(2):
                v = weights[6] * fg[0, r, col, part, :]
                for k in range(6):
                    v = v + weights[k] * fh[k, rows, lanes[col]]
                out[rows, lanes[col]] = v
            return carry

        lax.fori_loop(0, 8, mix, 0)
    for sem, ref in outgoing:
        wait(sem, ref)
    for s in range(NS):
        for r in range(2):
            here = jnp.logical_and(stays[r], jnp.logical_or(diagonal, near) if s < TURNED else diagonal)

            @pl.when(jnp.logical_not(here))
            def _():
                wait(t_send.at[s, r], pf.at[s, r])

    @pl.when(near)
    def _():
        wait(turn_send.at[0], turn)

    @pl.when(diagonal)
    def _():
        wait(hop_send.at[0], hop)


def body(fock_matrix, density, basis_gram, error_history, fock_history):
    any_ = pl.BlockSpec(memory_space=pl.ANY)
    v = lambda *shape: pltpu.VMEM(shape, F32)
    b = lambda *shape: pltpu.VMEM(shape, BF16)
    dma = pltpu.SemaphoreType.DMA
    block = pltpu.VMEM((512, 256), F32)
    next_, err, w = pl.pallas_call(
        kernel,
        out_shape=(block, block, pltpu.VMEM((1, 128), F32)),
        in_specs=[any_] * 5,
        out_specs=(pl.BlockSpec(memory_space=pltpu.VMEM),) * 3,
        scratch_shapes=[
            v(512, 256), v(4, NS, 64, 512), v(4, 2, 512, 128), v(4, 2, 2, 256, 128),
            b(NS, 256, 512), b(NS, 256, 512), b(NU, 512, 256), b(NU, 512, 256),
            b(NU, 2, 256, 256), b(NU, 2, 256, 256),
            v(NS, NU, 2, 4, 32, 256), v(NS, NU, 4, 32, 256),
            v(NS, NU, 2, 16, 256), v(NS, NU, 2, 32, 256),
            v(NS, NU, 2, 4, 32, 256), b(NS, NU, 256, 256), b(NS, NU, 256, 256),
            v(NS, 2, 4, 64, 256), v(NS, 2, 2, 32, 256), v(NS, 2, 2, 64, 256),
            v(NS, 2, 64, 256), v(NS, 2, 64, 256), v(NS, 2, 64, 256), v(TURNED, 2, 64, 256),
            v(6, 512, 256), v(6, 512, 256), v(512, 256),
            v(16, 24, 128), v(8, 24, 128), v(16, 8, 128), v(8, 8, 128),
            dma((18,)), dma((N_RECV,)), dma((9,)),
            dma((NS, 2)), dma((NS,)), dma((NS, 2)), dma((1,)), dma((TURNED,)), dma((1,)),
        ],
        compiler_params=pltpu.CompilerParams(
            collective_id=0, has_side_effects=True, vmem_limit_bytes=60 * 1024 * 1024
        ),
    )(fock_matrix, density, basis_gram, error_history, fock_history)
    return next_, err, w[0, :7]


def solution(mesh):
    split_mesh = Mesh(mesh.devices.reshape(4, 2, 4, 4), ("x", "c", "z", "y"))
    two = P(("x", "c"), ("z", "y"))
    three = P(None, ("x", "c"), ("z", "y"))
    return jax.shard_map(
        body,
        mesh=split_mesh,
        in_specs=(two, two, two, three, three),
        out_specs=(two, two, P()),
        check_vma=False,
    )
```

```python
import jax
import jax.numpy as jnp
from jax import lax
from jax.experimental import pallas as pl
from jax.experimental.pallas import tpu as pltpu
from jax.sharding import Mesh
from jax.sharding import PartitionSpec as P

MESH = pl.DeviceIdType.MESH
F32 = jnp.float32
BF16 = jnp.bfloat16
UNITS = (((0, 0), (0, 1)), ((1, 0), (2, 1)), ((1, 1), (2, 0)), ((3, 0), (3, 1)))
NS, NU = 4, 4
PAIRS = [(a, b) for a in range(6) for b in range(a, 6)]
GROUPS = (
    (0, 0, 1), (0, 1, 1), (1, 0, 2), (0, 2, 1), (0, 3, 1), (1, 2, 2), (2, 0, 2), (2, 2, 2), (3, 0, 2), (3, 2, 1),
    (3, 3, 1),
)
ORDER = (
    ("ys", 0), ("zs", 0), ("zs", 1), ("zf", 0), ("zf", 1), ("zs", 3), ("yf", 0), ("pd", 0), ("zs", 2), ("fs", 0),
    ("pd", 1), ("ps", 0), ("p0", 1), ("p0", 0), ("ps", 1), ("p0", 2), ("p1", 1), ("p1", 0), ("p1", 2), ("hist", 0),
    ("zf", 3), ("p2", 1), ("pd", 2), ("p2", 0), ("p0", 3), ("zf", 2), ("p2", 2), ("p1", 3), ("p3", 1), ("p3", 0),
    ("p3", 2), ("pd", 3), ("p0", 4), ("p0", 5), ("p2", 3), ("p4", 1), ("p1", 4), ("ps", 2), ("p4", 0), ("ps", 3),
    ("pf", 0, 0), ("p1", 5), ("p0", 7), ("ff", 0), ("p3", 3), ("p2", 4), ("p1", 7), ("p0", 6), ("fs", 1), ("p2", 5),
    ("p4", 2), ("p4", 3), ("p3", 4), ("p0", 10), ("p5", 0), ("p1", 6), ("p0", 9), ("p5", 1), ("pf", 1, 0), ("p3", 5),
    ("p6", 1, 0), ("p0", 8), ("p4", 4), ("p1", 9), ("p2", 7), ("p5", 3), ("ff", 1), ("pf", 0, 1), ("pf", 1, 1),
    ("pf", 3, 0), ("p6", 0, 0), ("p1", 10), ("p2", 6), ("pf", 2, 0), ("p4", 5), ("p5", 2), ("p1", 8), ("p5", 4),
    ("p6", 3, 0), ("p6", 4, 0), ("z1", 0, 0), ("p6", 0, 1), ("pf", 2, 1), ("p3", 7), ("p6", 1, 1), ("p2", 9),
    ("p6", 3, 1), ("pf", 3, 1), ("p6", 4, 1), ("z1", 0, 1), ("p3", 6), ("p5", 5), ("p2", 10), ("p6", 2, 0),
    ("p6", 2, 1), ("z2", 0, 0), ("p6", 5, 0), ("z1", 1, 0), ("p2", 8), ("p4", 7), ("p3", 9), ("z2", 0, 1),
    ("p6", 5, 1), ("z1", 1, 1), ("p4", 6), ("p3", 10), ("z2", 1, 0), ("p3", 8), ("z3", 0, 0), ("p5", 7), ("z3", 0, 1),
    ("ha",), ("p4", 9), ("z2", 1, 1), ("p5", 6), ("p6", 7, 0), ("p6", 7, 1), ("p4", 10), ("z3", 1, 0), ("p6", 6, 0),
    ("p6", 6, 1), ("p4", 8), ("z1", 2, 1), ("p5", 9), ("z3", 1, 1), ("z1", 2, 0), ("p5", 10), ("p6", 9, 0), ("p5", 8),
    ("p6", 10, 0), ("z2", 2, 1), ("p6", 10, 1), ("p6", 8, 0), ("z1", 3, 0), ("p6", 9, 1), ("u", 1), ("z2", 2, 0),
    ("p6", 8, 1), ("z1", 3, 1), ("t", 1, 1), ("u", 0), ("z2", 3, 0), ("z3", 2, 1), ("t", 0, 1), ("z2", 3, 1),
    ("t", 1, 0), ("z3", 2, 0), ("z3", 3, 0), ("t", 0, 0), ("z3", 3, 1), ("own",), ("t", 2, 1), ("t", 2, 0), ("u", 2),
    ("t", 3, 0), ("t", 3, 1), ("hb",),
)
N_RECV = 41 + 7 * len(GROUPS)
TURNED = 3


def split(v):
    hi = v.astype(BF16)
    return hi, (v - hi.astype(F32)).astype(BF16)


def dot3(a_hi, a_lo, b_hi, b_lo):
    a = jnp.concatenate([a_hi, a_hi, a_lo], axis=1)
    b = jnp.concatenate([b_hi, b_lo, b_hi], axis=0)
    return jnp.dot(a, b, preferred_element_type=F32)


def kernel(
    f_hbm, d_hbm, s_hbm, eh_hbm, fh_hbm, out, err, w_ref,
    s_in, sg, dg, fg, s_hi, s_lo, d_hi, d_lo, f_hi, f_lo,
    mp, dx, rab, flr, mf, m_hi, m_lo, pacc, zab, zlr, pf, tb, hop, turn,
    eh, fh, own, ha, hb, na, nb,
    send_sem, recv_sem, local_sem, t_send, t_recv, hop_recv, hop_send, turn_recv, turn_send,
):
    x, c, z, y = (lax.axis_index(n) for n in ("x", "c", "z", "y"))
    xr, xl, xo = lax.rem(x + 1, 4), lax.rem(x + 3, 4), lax.rem(x + 2, 4)
    dev = lambda x=x, c=c, z=z, y=y: (x, c, z, y)
    x_right, x_left = dev(x=xr), dev(x=xl)
    d_right, d_left = dev(z=lax.rem(z + 1, 4)), dev(z=lax.rem(z + 3, 4))
    s_right, s_left = dev(y=lax.rem(y + 1, 4)), dev(y=lax.rem(y + 3, 4))
    oc = 1 - c
    partner = dev(c=oc)

    used = {"send": 0, "recv": 0}
    outgoing = []

    def recv():
        used["recv"] += 1
        return recv_sem.at[used["recv"] - 1]

    def sender(*whole):
        used["send"] += len(whole)
        base = used["send"] - len(whole)
        for k, ref in enumerate(whole):
            outgoing.append((send_sem.at[base + k], ref))
        return [send_sem.at[base + k] for k in range(len(whole))]

    def send(src, dst, to, out_sem, in_sem):
        pltpu.make_async_remote_copy(
            src_ref=src, dst_ref=dst, send_sem=out_sem, recv_sem=in_sem, device_id=to, device_id_type=MESH,
        ).start()

    def wait(sem, ref):
        pltpu.make_async_copy(ref, ref, sem).wait()

    def load(k, *pairs):
        for src, dst in pairs:
            pltpu.make_async_copy(src, dst, local_sem.at[k]).start()


    lanes = [pl.ds(0, 128), pl.ds(128, 128)]
    halves = [pl.ds(0, 256), pl.ds(256, 256)]

    barrier = pltpu.get_barrier_semaphore()
    for to in (x_right, x_left, d_right, d_left, s_right, s_left, partner):
        pl.semaphore_signal(barrier, inc=1, device_id=to, device_id_type=MESH)
    load(0, (s_hbm, s_in))
    load(1, *((d_hbm.at[:, lanes[h]], dg.at[0, h]) for h in range(2)))
    load(2, (eh_hbm, eh))
    load(3, *((f_hbm.at[halves[r], lanes[h]], fg.at[0, r, h]) for r in range(2) for h in range(2)))
    load(4, (fh_hbm, fh))
    wait(local_sem.at[0], s_in)
    for n in range(2):
        for k in range(4):
            block = s_in[pl.ds(128 * k, 128), lanes[n]].T
            for e in range(2):
                sg[0, 2 * n + e, :, pl.ds(128 * k, 128)] = block[64 * e : 64 * (e + 1)]
    pl.semaphore_wait(barrier, 7)

    three = pl.ds(0, 3)
    (d_out,) = sender(dg.at[three])
    (f_out,) = sender(fg.at[three])
    (s_out,) = sender(sg.at[three])

    class Line:
        def __init__(self, src, slot, size, right, left, out_sem):
            self.src, self.slot, self.size, self.right, self.left, self.out = src, slot, size, right, left, out_sem
            self.sems = [recv() for _ in range(3)]

        def begin(self):
            a, b, _ = self.sems
            send(self.src(0), self.slot(1, 0), self.right, self.out, a)
            send(self.src(1), self.slot(2, 1), self.left, self.out, a)
            send(self.src(1), self.slot(1, 1), self.right, self.out, b)
            send(self.src(0), self.slot(2, 0), self.left, self.out, b)

        def forward(self):
            wait(self.sems[0], self.size)
            send(self.slot(1, 0), self.slot(3, 0), self.right, self.out, self.sems[2])
            send(self.slot(2, 1), self.slot(3, 1), self.left, self.out, self.sems[2])

        def second(self):
            wait(self.sems[1], self.size)

        def third(self):
            wait(self.sems[2], self.size)

    d_line = Line(lambda h: d_hbm.at[:, lanes[h]], lambda slot, h: dg.at[slot, h], dg.at[1], d_right, d_left, d_out)
    f_line = [
        Line(
            lambda h, r=r: f_hbm.at[halves[r], lanes[h]], lambda slot, h, r=r: fg.at[slot, r, h],
            fg.at[1, r], d_right, d_left, f_out,
        )
        for r in range(2)
    ]

    LO, HI = pl.ds(0, 32), pl.ds(32, 32)
    part = (LO, HI)
    s_line = [
        Line(
            lambda h, s=s: sg.at[0, s, part[h]], lambda slot, h, s=s: sg.at[slot, s, part[h]],
            sg.at[1, s], s_right, s_left, s_out,
        )
        for s in range(NS)
    ]

    def prep_s(s, slots):
        for slot in slots:
            hi, lo = split(sg[slot, s])
            at = pl.ds(64 * slot, 64)
            s_hi[s, at, :] = hi
            s_lo[s, at, :] = lo

    def prep_d(u):
        for n, (slot, h) in enumerate(UNITS[u]):
            hi, lo = split(dg[slot, h])
            d_hi[u, :, lanes[n]] = hi
            d_lo[u, :, lanes[n]] = lo

    def prep_f(u, r):
        for n, (slot, h) in enumerate(UNITS[u]):
            for k in range(2):
                hi, lo = split(fg[slot, r, h, lanes[k], :].T)
                f_hi[u, r, lanes[n], lanes[k]] = hi
                f_lo[u, r, lanes[n], lanes[k]] = lo

    TOP, LOW = pl.ds(0, 16), pl.ds(16, 16)
    g = [dict() for _ in GROUPS]

    def at(n):
        s, first, count = GROUPS[n]
        return s, pl.ds(first, count), range(first, first + count)

    dx_out, r_out, f1_out, f0_out, g_right, g_left, h_out, q_out = sender(
        dx, rab, flr.at[:, :, 0], flr.at[:, :, 1], flr.at[:, :, 0], flr.at[:, :, 0], flr.at[:, :, 0], dx
    )

    def p0(n):
        s, us, units = at(n)
        d = [jnp.concatenate([ref[u] for u in units], axis=1) for ref in (d_hi, d_lo)]
        tile = dot3(s_hi[s], s_lo[s], *d)
        for k, u in enumerate(units):
            mp[s, u] = tile[:, 256 * k : 256 * (k + 1)].reshape(2, 4, 32, 256)
        for name in ("dx", "r", "f", "g1", "g2", "h", "q"):
            g[n][name] = recv()
        send(mp.at[s, us, oc], dx.at[s, us], partner, dx_out, g[n]["dx"])

    def p1(n):
        s, us, _ = at(n)
        wait(g[n]["dx"], dx.at[s, us])
        mp[s, us, c] += dx[s, us]
        send(mp.at[s, us, c, xo, TOP], rab.at[s, us, 0], x_right, r_out, g[n]["r"])
        send(mp.at[s, us, c, xo, LOW], rab.at[s, us, 1], x_left, r_out, g[n]["r"])
        send(mp.at[s, us, c, xr, LOW], flr.at[s, us, 0, LOW], x_right, f1_out, g[n]["f"])
        send(mp.at[s, us, c, xl, TOP], flr.at[s, us, 1, TOP], x_left, f1_out, g[n]["f"])

    def p2(n):
        s, us, _ = at(n)
        wait(g[n]["r"], rab.at[s, us])
        mp[s, us, c, xr, TOP] += rab[s, us, 0]
        send(mp.at[s, us, c, xr, TOP], flr.at[s, us, 0, TOP], x_right, f0_out, g[n]["f"])
        mp[s, us, c, xl, LOW] += rab[s, us, 1]
        send(mp.at[s, us, c, xl, LOW], flr.at[s, us, 1, LOW], x_left, f0_out, g[n]["f"])

    def p3(n):
        s, us, _ = at(n)
        wait(g[n]["f"], flr.at[s, us])
        mf[s, us, c, x] = mp[s, us, c, x] + flr[s, us, 0] + flr[s, us, 1]
        top, low, whole = mf.at[s, us, c, x, TOP], mf.at[s, us, c, x, LOW], mf.at[s, us, c, x]
        send(top, top, x_right, g_right, g[n]["g1"])
        send(low, low, x_left, g_left, g[n]["g1"])
        send(low, low, x_right, g_right, g[n]["g2"])
        send(top, top, x_left, g_left, g[n]["g2"])
        send(whole, whole, partner, q_out, g[n]["q"])

    def p4(n):
        s, us, _ = at(n)
        left, right = mf.at[s, us, c, xl], mf.at[s, us, c, xr]
        left_top, right_low = mf.at[s, us, c, xl, TOP], mf.at[s, us, c, xr, LOW]
        wait(g[n]["g1"], left)
        send(left_top, left_top, x_right, h_out, g[n]["h"])
        send(right_low, right_low, x_left, h_out, g[n]["h"])
        wait(g[n]["g2"], left)
        send(left, left, partner, q_out, g[n]["q"])
        send(right, right, partner, q_out, g[n]["q"])

    def p5(n):
        s, us, _ = at(n)
        wait(g[n]["h"], mf.at[s, us, c, xo])
        send(mf.at[s, us, c, xo], mf.at[s, us, c, xo], partner, q_out, g[n]["q"])

    begun = set()

    def p6(n, r):
        s, us, units = at(n)
        if "done" not in g[n]:
            wait(g[n]["q"], mf.at[s, us, oc])
            for u in units:
                m_hi[s, u], m_lo[s, u] = split(mf[s, u].reshape(256, 256))
            g[n]["done"] = True
        m = [jnp.concatenate([ref[s, u] for u in units], axis=1) for ref in (m_hi, m_lo)]
        f = [jnp.concatenate([ref[u, r] for u in units], axis=0) for ref in (f_hi, f_lo)]
        part = dot3(*m, *f).reshape(4, 64, 256)
        if (s, r) in begun:
            pacc[s, r] += part
        else:
            pacc[s, r] = part
            begun.add((s, r))

    w = {(s, r): (recv(), recv()) for s in range(NS) for r in range(2)}
    za_out, z1_out, z0_out = sender(zab, zlr.at[:, :, 0], zlr.at[:, :, 0])

    def z1(s, r):
        a, f = w[s, r]
        send(pacc.at[s, r, 3, LO], zab.at[s, r, 0], s_right, za_out, a)
        send(pacc.at[s, r, 3, HI], zab.at[s, r, 1], s_left, za_out, a)
        send(pacc.at[s, r, 2, HI], zlr.at[s, r, 0, HI], s_right, z1_out, f)
        send(pacc.at[s, r, 1, LO], zlr.at[s, r, 1, LO], s_left, z1_out, f)

    def z2(s, r):
        a, f = w[s, r]
        wait(a, zab.at[s, r])
        pacc[s, r, 2, LO] += zab[s, r, 0]
        send(pacc.at[s, r, 2, LO], zlr.at[s, r, 0, LO], s_right, z0_out, f)
        pacc[s, r, 1, HI] += zab[s, r, 1]
        send(pacc.at[s, r, 1, HI], zlr.at[s, r, 1, HI], s_left, z0_out, f)

    parity = lax.rem(y, 2)
    t_core = lax.div(y, 2)
    apart = lax.rem(x - z + 4, 4)
    diagonal, far = apart == 0, apart == 2
    near = jnp.logical_or(apart == 1, apart == 3)
    stays = [jnp.logical_and(c == t_core, parity == r) for r in range(2)]

    def t_first(s, r):
        end, in_plane = (tb.at[s, parity], t_recv.at[s]), (x, t_core, z, 2 * c + r)
        yield diagonal, stays[r], *end, in_plane
        yield far, None, hop.at[s, r], hop_recv.at[s, r], dev(z=x)
        if s < TURNED:
            yield near, stays[r], turn.at[s, parity], turn_recv.at[s], in_plane
        else:
            yield near, None, *end, (z, t_core, x, 2 * c + r)

    def t_copy(s, r, dst, sem, to):
        return pltpu.make_async_remote_copy(
            src_ref=pf.at[s, r], dst_ref=dst, send_sem=t_send.at[s, r], recv_sem=sem, device_id=to, device_id_type=MESH,
        )

    def z3(s, r):
        wait(w[s, r][1], zlr.at[s, r])
        pf[s, r] = pacc[s, r, 0] + zlr[s, r, 0] + zlr[s, r, 1]
        for case, local_case, dst, sem, to in t_first(s, r):
            away = case if local_case is None else jnp.logical_and(case, jnp.logical_not(local_case))

            @pl.when(away)
            def _(dst=dst, sem=sem, to=to):
                t_copy(s, r, dst, sem, to).start()

            if local_case is not None:

                @pl.when(jnp.logical_and(case, local_case))
                def _(dst=dst, sem=sem):
                    pltpu.make_async_copy(pf.at[s, r], dst, sem).start()

    def pass_on(s):
        @pl.when(near)
        def _():
            wait(turn_recv.at[s], turn.at[s])
            send(turn.at[s], tb.at[s], dev(x=z, z=x), turn_send.at[0], t_recv.at[s])

    def relay(s, r):
        @pl.when(diagonal)
        def _():
            wait(hop_recv.at[s, r], hop.at[s, r])
            send(hop.at[s, r], tb.at[s, parity], (xo, t_core, x, 2 * c + r), hop_send.at[0], t_recv.at[s])

    def turn_own():
        for n in range(2):
            for r in range(2):
                own[halves[r], lanes[n]] = jnp.concatenate([pf[2 * n, r], pf[2 * n + 1, r]], axis=0).T

    def history_gram():
        def step(n, acc):
            rows = pl.ds(pl.multiple_of(8 * n, 8), 8)
            acc = list(acc)
            for col in range(2):
                e = [eh[k, rows, lanes[col]] for k in range(6)]
                acc = [v + e[a] * e[b] for v, (a, b) in zip(acc, PAIRS)]
            return tuple(acc)

        acc = lax.fori_loop(0, 64, step, tuple(jnp.zeros((8, 128), F32) for _ in PAIRS))
        return [jnp.sum(v, axis=0, keepdims=True) for v in acc]

    plane, line = 4 * z + y, 2 * x + c
    sum_out = {n: sender(a.at[pl.ds(0, 15)], b.at[pl.ds(0, 7)]) for n, (a, b) in enumerate(((ha, hb), (na, nb)))}
    sum_in = {n: (recv(), recv()) for n in range(2)}

    def sum_plane(n, ref, rows):
        ref[plane] = jnp.concatenate(rows, axis=0)
        for d in range(1, 16):
            to = lax.rem(plane + d, 16)
            send(ref.at[plane], ref.at[plane], dev(z=lax.div(to, 4), y=lax.rem(to, 4)), sum_out[n][0], sum_in[n][0])

    def added(ref, count):
        total = ref[0]
        for k in range(1, count):
            total = total + ref[k]
        return total

    def sum_line(n, ref, before):
        wait(sum_in[n][0], before.at[pl.ds(0, 15)])
        ref[line] = added(before, 16)
        for d in range(1, 8):
            to = lax.rem(line + d, 8)
            send(ref.at[line], ref.at[line], dev(x=lax.div(to, 2), c=lax.rem(to, 2)), sum_out[n][1], sum_in[n][1])

    def sum_end(n, ref):
        wait(sum_in[n][1], ref.at[pl.ds(0, 7)])
        total = jnp.sum(added(ref, 8), axis=1, keepdims=True)
        return jnp.broadcast_to(total, (total.shape[0], 128))

    hist = []

    def first_gram():
        wait(local_sem.at[2], eh)
        hist.extend(history_gram() + [jnp.zeros((3, 128), F32)])

    def do_ps(s):
        s_line[s].second()
        s_line[s].third()
        prep_s(s, (0, 1, 2, 3))

    def do_pd(u):
        if u == 0:
            wait(local_sem.at[1], dg.at[0])
        if u == 2:
            d_line.second()
        if u == 3:
            d_line.third()
        prep_d(u)

    def do_pf(u, r):
        if u == 0 and r == 0:
            wait(local_sem.at[3], fg.at[0])
        if u == 2:
            f_line[r].second()
        if u == 3:
            f_line[r].third()
        prep_f(u, r)

    work = {
        "ys": lambda _: d_line.begin(), "yf": lambda _: d_line.forward(),
        "fs": lambda r: f_line[r].begin(), "ff": lambda r: f_line[r].forward(),
        "zs": lambda s: s_line[s].begin(), "zf": lambda s: s_line[s].forward(),
        "ps": do_ps, "pd": do_pd, "pf": do_pf, "hist": lambda _: first_gram(),
        "p0": p0, "p1": p1, "p2": p2, "p3": p3, "p4": p4, "p5": p5, "p6": p6,
        "z1": z1, "z2": z2, "z3": z3, "t": relay, "u": pass_on, "own": turn_own,
        "ha": lambda: sum_plane(0, ha, hist), "hb": lambda: sum_line(0, hb, ha),
    }
    for phase, *where in ORDER:
        work[phase](*where)

    wait(local_sem.at[4], fh)
    sums = [jnp.zeros((8, 128), F32) for _ in range(7)]
    for s in range(NS):
        wait(t_recv.at[s], tb.at[s])
        for half in range(2):
            start = 256 * half + 64 * s

            def step(n, acc):
                rows = pl.ds(pl.multiple_of(start + 32 * n, 32), 32)
                for col in range(2):
                    e = own[rows, lanes[col]] - tb[s, half, pl.ds(pl.multiple_of(32 * n, 32), 32), lanes[col]]
                    err[rows, lanes[col]] = e
                    terms = [eh[k, rows, lanes[col]] * e for k in range(6)] + [e * e]
                    acc = tuple(v + jnp.sum(t.reshape(4, 8, 128), axis=0) for v, t in zip(acc, terms))
                return acc

            sums = lax.fori_loop(0, 2, step, tuple(sums))

    sum_plane(1, na, [jnp.sum(v, axis=0, keepdims=True) for v in sums] + [jnp.zeros((1, 128), F32)])
    sum_line(1, nb, na)
    hist.append(sum_end(0, hb))
    new = sum_end(1, nb)

    gram = {}
    for n, (a, b) in enumerate(PAIRS):
        gram[b, a] = hist[-1][n : n + 1]
    for k in range(7):
        gram[6, k] = new[k : k + 1]
    low = {}
    for j in range(7):
        v = gram[j, j]
        for k in range(j):
            v = v - low[j, k] * low[j, k]
        low[j, j] = jnp.sqrt(v)
        for i in range(j + 1, 7):
            v = gram[i, j]
            for k in range(j):
                v = v - low[i, k] * low[j, k]
            low[i, j] = v / low[j, j]
    forward = []
    for i in range(7):
        v = jnp.ones((1, 128), F32)
        for k in range(i):
            v = v - low[i, k] * forward[k]
        forward.append(v / low[i, i])
    backward = [None] * 7
    for i in range(6, -1, -1):
        v = forward[i]
        for k in range(i + 1, 7):
            v = v - low[k, i] * backward[k]
        backward[i] = v / low[i, i]
    norm = backward[0]
    for v in backward[1:]:
        norm = norm + v
    weights = [v / norm for v in backward]
    lane = lax.broadcasted_iota(jnp.int32, (1, 128), 1)
    row = jnp.zeros((1, 128), F32)
    for k in range(7):
        row = jnp.where(lane == k, weights[k], row)
    w_ref[...] = row

    for r in range(2):

        def mix(n, carry):
            part = pl.ds(pl.multiple_of(32 * n, 32), 32)
            rows = pl.ds(pl.multiple_of(256 * r + 32 * n, 32), 32)
            for col in range(2):
                v = weights[6] * fg[0, r, col, part, :]
                for k in range(6):
                    v = v + weights[k] * fh[k, rows, lanes[col]]
                out[rows, lanes[col]] = v
            return carry

        lax.fori_loop(0, 8, mix, 0)
    for sem, ref in outgoing:
        wait(sem, ref)
    for s in range(NS):
        for r in range(2):
            here = jnp.logical_and(stays[r], jnp.logical_or(diagonal, near) if s < TURNED else diagonal)

            @pl.when(jnp.logical_not(here))
            def _():
                wait(t_send.at[s, r], pf.at[s, r])

    @pl.when(near)
    def _():
        wait(turn_send.at[0], turn)

    @pl.when(diagonal)
    def _():
        wait(hop_send.at[0], hop)


def body(fock_matrix, density, basis_gram, error_history, fock_history):
    any_ = pl.BlockSpec(memory_space=pl.ANY)
    v = lambda *shape: pltpu.VMEM(shape, F32)
    b = lambda *shape: pltpu.VMEM(shape, BF16)
    dma = pltpu.SemaphoreType.DMA
    block = pltpu.VMEM((512, 256), F32)
    next_, err, w = pl.pallas_call(
        kernel,
        out_shape=(block, block, pltpu.VMEM((1, 128), F32)),
        in_specs=[any_] * 5,
        out_specs=(pl.BlockSpec(memory_space=pltpu.VMEM),) * 3,
        scratch_shapes=[
            v(512, 256), v(4, NS, 64, 512), v(4, 2, 512, 128), v(4, 2, 2, 256, 128),
            b(NS, 256, 512), b(NS, 256, 512), b(NU, 512, 256), b(NU, 512, 256),
            b(NU, 2, 256, 256), b(NU, 2, 256, 256),
            v(NS, NU, 2, 4, 32, 256), v(NS, NU, 4, 32, 256),
            v(NS, NU, 2, 16, 256), v(NS, NU, 2, 32, 256),
            v(NS, NU, 2, 4, 32, 256), b(NS, NU, 256, 256), b(NS, NU, 256, 256),
            v(NS, 2, 4, 64, 256), v(NS, 2, 2, 32, 256), v(NS, 2, 2, 64, 256),
            v(NS, 2, 64, 256), v(NS, 2, 64, 256), v(NS, 2, 64, 256), v(TURNED, 2, 64, 256),
            v(6, 512, 256), v(6, 512, 256), v(512, 256),
            v(16, 24, 128), v(8, 24, 128), v(16, 8, 128), v(8, 8, 128),
            dma((18,)), dma((N_RECV,)), dma((5,)),
            dma((NS, 2)), dma((NS,)), dma((NS, 2)), dma((1,)), dma((TURNED,)), dma((1,)),
        ],
        compiler_params=pltpu.CompilerParams(
            collective_id=0, has_side_effects=True, vmem_limit_bytes=60 * 1024 * 1024
        ),
    )(fock_matrix, density, basis_gram, error_history, fock_history)
    return next_, err, w[0, :7]


def solution(mesh):
    split_mesh = Mesh(mesh.devices.reshape(4, 2, 4, 4), ("x", "c", "z", "y"))
    two = P(("x", "c"), ("z", "y"))
    three = P(None, ("x", "c"), ("z", "y"))
    return jax.shard_map(
        body,
        mesh=split_mesh,
        in_specs=(two, two, two, three, three),
        out_specs=(two, two, P()),
        check_vma=False,
    )
```
